32 devices in a mesh: chain: 8 (over z, core), bond: 4 (over y, x).
Axes of the slice: x: 2, y: 2, z: 4, core: 2. Of those that a mesh axis runs over, the one named last changes fastest.
Arguments:
- site_tensors: float32 [32, 256, 2, 256], P('chain', 'bond'), may hold values from -20 to 20
- bond_gates: float32 [32, 4, 4], P('chain'), may hold values from -1.5 to 2.5
Outputs:
- state: float32 [32, 256, 2, 256], P('chain', 'bond')
- profile: float32 [32], P('chain')
The draws below stay inside these ranges and needn't reach their ends.
All inputs are finite; a program needn't handle non-finite values.
Results may differ from the reference program's by a relative error of at most 0.0002.
Values sent between devices are 32-bit elements; how exact they have to be, the bound alone decides.
A program may use at most 64 MiB of HBM per device.

```python
import math
import jax
import jax.numpy as jnp
from jax import lax

CHI = 256
NS_ITERS = 3
SITES = 32


def draw_site_tensors(key, part):
    key_base = jax.random.fold_in(key, 11)
    shape = (SITES, CHI, 2, CHI)
    base = jnp.clip(jax.random.normal(key_base, shape, jnp.float32), -6.0, 6.0)
    ramp = jnp.exp(-2.0 * jnp.arange(SITES, dtype=jnp.float32) / SITES)
    return base * ramp[:, None, None, None]


def draw_bond_gates(key, part):
    key_noise = jax.random.fold_in(key, 21)
    noise = 0.3 * jnp.clip(jax.random.normal(key_noise, (SITES, 4, 4), jnp.float32), -4.0, 4.0)
    return jnp.eye(4, dtype=jnp.float32)[None, :, :] + noise


def setup_inputs(seed: int = 0) -> dict:
    key_list = jax.random.split(jax.random.key(seed), 3)
    return {
        "site_tensors": draw_site_tensors(jax.random.fold_in(key_list[2], 71), 0),
        "bond_gates": draw_bond_gates(jax.random.fold_in(key_list[2], 71), 0),
    }


epsilon = 1e-06
exact = lax.Precision.HIGHEST

def bond_update(operands):
    left, right, gate = operands
    width = left.shape[0]
    two_site = jnp.einsum('asm,mtb->astb', left, right, precision=exact) / math.sqrt(width)
    gated = jnp.einsum('stuv,auvb->astb', gate.reshape(2, 2, 2, 2), two_site, precision=exact)
    matrix = gated.reshape(2 * width, 2 * width)
    projected = jnp.dot(matrix, right.reshape(width, 2 * width).T, precision=exact)
    squares = jnp.sum(projected * projected)
    iterate = projected / jnp.sqrt(squares + epsilon)
    for repeat in range(NS_ITERS):
        gram = jnp.dot(iterate.T, iterate, precision=exact)
        iterate = 1.5 * iterate - 0.5 * jnp.dot(iterate, gram, precision=exact)
    carried = jnp.dot(iterate.T, matrix, precision=exact)
    scale_norm = jnp.sqrt(jnp.mean(carried * carried) + epsilon)
    new_left = (math.sqrt(2 * width) * iterate).reshape(width, 2, width)
    new_right = (carried / scale_norm).reshape(width, 2, width)
    return (new_left, new_right, jnp.log(scale_norm))

def reference(site_tensors, bond_gates):
    sites = site_tensors.shape[0]
    new_left, new_right, weights_even = lax.map(bond_update, (site_tensors[0::2], site_tensors[1::2], bond_gates[0::2]))
    half_state = jnp.stack([new_left, new_right], axis=1).reshape(site_tensors.shape)
    rolled = jnp.roll(half_state, -1, axis=0)
    new_left, new_right, weights_odd = lax.map(bond_update, (half_state[1::2], rolled[1::2], bond_gates[1::2]))
    even_sites = jnp.roll(new_right, 1, axis=0)
    state = jnp.stack([even_sites, new_left], axis=1).reshape(site_tensors.shape)
    weights = jnp.stack([weights_even, weights_odd], axis=1).reshape(sites)
    profile = jnp.cumsum(weights) / sites
    return (state, profile)
```

```python
import functools
import math

import jax
import jax.numpy as jnp
from jax import lax
from jax.experimental import pallas as pl
from jax.experimental.pallas import tpu as pltpu
from jax.sharding import PartitionSpec as P

NS_ITERS = 3
RING = 4
GROUPS = 4
LANES = 128
EPSILON = 1e-06


def split(value):
    high = value.astype(jnp.bfloat16)
    low = (value - high.astype(jnp.float32)).astype(jnp.bfloat16)
    return (high, low)


def dot(a, b):
    return jnp.dot(a, b, preferred_element_type=jnp.float32)


def dot_t(a, b):
    return lax.dot_general(a, b, (((1,), (1,)), ((), ())), preferred_element_type=jnp.float32)


def times(a, b):
    (ah, al), (bh, bl) = (a, b)
    return dot(ah, bh) + dot(al, bh) + dot(ah, bl)


def times_transposed(a, b):
    (ah, al), (bh, bl) = (a, b)
    return dot_t(ah, bh) + dot_t(al, bh) + dot_t(ah, bl)


def mixed(theta, gate, width):
    r = theta.shape[0] // 2
    theta = [[theta[u * r:(u + 1) * r, v * width:(v + 1) * width] for v in range(2)] for u in range(2)]
    scaled = gate * (1.0 / math.sqrt(width))
    rows = []
    for s in range(2):
        row = []
        for t in range(2):
            total = None
            for u in range(2):
                for v in range(2):
                    factor = scaled[2 * s + t:2 * s + t + 1, 2 * u + v:2 * u + v + 1]
                    term = factor * theta[u][v]
                    total = term if total is None else total + term
            row.append(total)
        rows.append(jnp.concatenate(row, axis=1))
    return jnp.concatenate(rows, axis=0)


def newton_schulz(gram, fill=()):
    assert NS_ITERS == 3
    fill = list(fill)

    def filled(value):
        if fill:
            fill.pop(0)()
        return value

    eye = jnp.where(
        lax.broadcasted_iota(jnp.int32, gram.shape, 0) == lax.broadcasted_iota(jnp.int32, gram.shape, 1),
        jnp.float32(1.5),
        jnp.float32(0.0),
    )
    factor = None
    for repeat in range(NS_ITERS):
        step = eye - 0.5 * gram
        factor = step if factor is None else times(split(factor), split(step))
        if repeat < NS_ITERS - 1:
            gram_split = split(gram)
            once = 1.5 * gram - 0.5 * filled(times(gram_split, gram_split))
            gram = 1.5 * once - 0.5 * filled(times(split(once), gram_split))
    while fill:
        fill.pop(0)()
    return split(factor)


def sum_of_squares(value):
    return jnp.sum(value * value, keepdims=True)


def norm_of(carried):
    mean = sum_of_squares(carried) * (1.0 / carried.size)
    return jnp.sqrt(mean + EPSILON)


def order(place):
    return place + (place // 2) * (1 - 2 * (place % 2))


def grouped(mine, d):
    if d == 0:
        return mine
    if d == 1:
        return mine + 1 - 2 * (mine % 2)
    if d == 2:
        return lax.rem(mine + 2, 4)
    return 3 - mine


def kernel(
    chains, bonds, rows, width,
    x_ref, gates_ref, out_ref, profile_ref,
    slab_sem, ring_sem, fetch_sem, xin, inbuf, gates, rsend, rrecv, obuf, wall,
    bh, bl, th, tl, mh, ml, ph, pl_, lh, ll, nh, nl, uh, ul, kept,
    g_send, g_recv, f_send, f_recv, gate_send, gate_recv,
    m_send, m_recv, h_send, h_recv, o_send, o_recv, w_send, w_recv,
):
    chain, bond = (lax.axis_index("chain"), lax.axis_index("bond"))
    slabs = chains // 2
    slab, core = (chain // 2, chain % 2)
    tall = rows * 4
    sibling = {"chain": 2 * slab + 1 - core, "bond": bond}
    replica = bond // RING

    def place_of(ring_at, slab_at):
        return order(lax.rem(ring_at + 3 * slab_at, RING))

    ring = lax.rem(order(bond % RING) + slab, RING)

    def remote(src, dst, send, recv_sem, chain_to, bond_to):
        return pltpu.make_async_remote_copy(
            src_ref=src, dst_ref=dst, send_sem=send, recv_sem=recv_sem,
            device_id={"chain": chain_to, "bond": bond_to},
            device_id_type=pl.DeviceIdType.MESH,
        )

    def landed(ref, sem):
        pltpu.make_async_copy(ref, ref, sem).wait()

    fetch = pltpu.make_async_copy(x_ref, xin, fetch_sem)
    fetch.start()
    gate_here = pltpu.make_async_copy(gates_ref, gates.at[core], gate_recv.at[core])
    gate_here.start()
    barrier = pltpu.get_barrier_semaphore()

    def greet(semaphore, chain_to, bond_to):
        to = {"chain": chain_to, "bond": bond_to}
        pl.semaphore_signal(semaphore, inc=1, device_id=to, device_id_type=pl.DeviceIdType.MESH)

    for db in range(1, bonds):
        greet(barrier, 2 * slab + 1, lax.rem(bond + db, bonds))

    @pl.when(core == 0)
    def _():
        greet(barrier, 2 * slab + 1, bond)

    for dz in range(1, slabs):
        for db in range(RING):
            greet(barrier, 2 * lax.rem(slab + dz, slabs), replica * RING + lax.rem(bond + db, RING))

    @pl.when(core == 1)
    def _():
        pl.semaphore_wait(barrier, 2 * bonds - 1)
        greet(slab_sem, 2 * slab, bond)

    @pl.when(core == 0)
    def _():
        pl.semaphore_wait(slab_sem, 1)

    gate_copy = remote(gates_ref, gates.at[core], gate_send, gate_recv.at[core], sibling["chain"], bond)
    gate_copy.start()
    fetch.wait()

    short = tall // 2
    gathers = []
    for i in (1, 0):
        for h in range(2):
            for j in range(2):
                for r in range(bonds // RING):
                    bond_to = r * RING + place_of(2 * core + j, slab)
                    src = xin.at[pl.ds((2 * j + i) * tall + h * short, short)]
                    dst = inbuf.at[i, pl.ds(bond * tall + h * short, short)]
                    sem = g_recv.at[i, bond]
                    copy = remote(src, dst, g_send.at[i, h, j, r], sem, 2 * slab + h, bond_to)
                    here = pltpu.make_async_copy(src, dst, sem)
                    mine = jnp.logical_and(core == h, bond_to == bond)
                    gathers.append((copy, mine))
                    pl.when(mine)(here.start)
                    pl.when(jnp.logical_not(mine))(copy.start)

    forwards = []
    part = bonds // GROUPS
    tier = width // GROUPS

    def members(d):
        return [grouped(bond // part, d) * part + lax.rem(bond + e, part) for e in range(part)]

    def pass_on(i, d):
        for origin in members(d):
            piece = inbuf.at[i, pl.ds(origin * tall + core * short, short)]
            landed(piece, g_recv.at[i, origin])
            copy = remote(
                piece, piece, f_send.at[i, origin], f_recv.at[i, origin], sibling["chain"], bond
            )
            copy.start()
            forwards.append(copy)

    def complete(i, d):
        for origin in members(d):
            landed(inbuf.at[i, pl.ds(origin * tall + (1 - core) * short, short)], f_recv.at[i, origin])

    def spin(i, s, row, count):
        return jnp.concatenate(
            [inbuf[i, pl.ds(4 * row + 2 * t + s, count, stride=4), :] for t in range(2)], axis=1
        )

    block = ring // 2
    before = lax.rem(ring + RING - 1, RING)
    slab_to = lax.rem(slab + slabs - jnp.where(ring == 0, 1, 0), slabs)
    prev_bond = replica * RING + place_of(before, slab_to)
    after = lax.rem(ring + 1, RING)
    slab_from = lax.rem(slab + jnp.where(ring == RING - 1, 1, 0), slabs)
    next_bond = replica * RING + place_of(after, slab_from)

    pass_on(1, 0)
    pass_on(0, 0)
    for d in range(1, GROUPS):
        pass_on(1, d)
    for d in range(GROUPS):
        complete(1, d)
    landed(gates.at[0], gate_recv.at[0])
    landed(gates.at[1], gate_recv.at[1])
    right = jnp.concatenate([spin(1, s, 0, width) for s in range(2)], axis=1)
    bh[...], bl[...] = split(right)
    th[...], tl[...] = split(right.T)

    @pl.when(core == 0)
    def _():
        pl.semaphore_wait(barrier, (slabs - 1) * 2 * RING)
        greet(ring_sem, 2 * slab + 1, bond)

    @pl.when(core == 1)
    def _():
        pl.semaphore_wait(ring_sem, 1)

    gate = gates[block, 2 * (ring % 2)]
    passed = []
    squares = None
    for d in range(GROUPS):
        g = grouped(bond // part, d)
        if d == 1:
            pass_on(0, 1)
            pass_on(0, 2)
        if d == 2:
            pass_on(0, 3)
        complete(0, d)
        left = jnp.concatenate([spin(0, s, g * tier, tier) for s in range(2)], axis=0)
        theta = times(split(left), (bh[...], bl[...]))
        matrix = split(mixed(theta, gate, width))
        here = pl.ds(d * 2 * tier, 2 * tier)
        mh[here, :], ml[here, :] = matrix
        projected = times(matrix, (th[...], tl[...]))
        for s in range(2):
            rsend[s, pl.ds(g * tier, tier)] = projected[s * tier:(s + 1) * tier]
        piece = pl.ds(g * tier, tier)
        copy = remote(
            rsend.at[core, piece], rrecv.at[core, piece], m_send.at[d], m_recv.at[d],
            2 * slab_to + core, prev_bond,
        )
        copy.start()
        passed.append(copy)
        square = sum_of_squares(projected)
        squares = square if squares is None else squares + square
        ph[:, here], pl_[:, here] = split(projected.T)

    turned = (ph[...], pl_[...])
    inverse = 1.0 / (squares + EPSILON)
    gram = times_transposed(turned, turned) * inverse
    root = jnp.sqrt(inverse)

    def carry_even(q):
        here = slice(q * width, (q + 1) * width)
        kept[:, here] = times(turned, (mh[:, here], ml[:, here])) * root

    factor = newton_schulz(gram, [functools.partial(carry_even, q) for q in range(2)])
    carried = times(factor, split(kept[...]))
    scale_norm = norm_of(carried)
    weight_even = jnp.log(scale_norm)
    carried = split(carried * (1.0 / scale_norm))
    for s in range(2):
        lh[s * width:(s + 1) * width, :] = carried[0][:, s * width:(s + 1) * width]
        ll[s * width:(s + 1) * width, :] = carried[1][:, s * width:(s + 1) * width]

    gram = None
    squares = None
    for d in range(GROUPS):
        piece = rrecv.at[core, pl.ds(grouped(next_bond // part, d) * tier, tier)]
        landed(piece, m_recv.at[d])
        copy = remote(piece, piece, h_send.at[d], h_recv.at[d], sibling["chain"], bond)
        copy.start()
        forwards.append(copy)
        if d % 2 == 0:
            continue
        parts = []
        for e in (d - 1, d):
            g = grouped(next_bond // part, e)
            landed(rrecv.at[1 - core, pl.ds(g * tier, tier)], h_recv.at[e])
            for s in range(2):
                parts.append(rrecv[s, pl.ds(g * tier, tier)])
        received = jnp.concatenate(parts, axis=0)
        square = sum_of_squares(received)
        squares = square if squares is None else squares + square
        turned = split(received.T)
        piece = split(received)
        for k, (e, s) in enumerate([(e, s) for e in (d - 1, d) for s in range(2)]):
            g = grouped(next_bond // part, e)
            nh[pl.ds(s * width + g * tier, tier), :] = piece[0][k * tier:(k + 1) * tier]
            nl[pl.ds(s * width + g * tier, tier), :] = piece[1][k * tier:(k + 1) * tier]
        product = times(turned, piece)
        gram = product if gram is None else gram + product
    inverse = 1.0 / (squares + EPSILON)
    gate = gates[block, 2 * (ring % 2) + 1]
    half = width // 2

    def ahead(q):
        left = tuple(
            jnp.concatenate([ref[s * width + q * half:s * width + (q + 1) * half, :] for s in range(2)], axis=0)
            for ref in (lh, ll)
        )
        theta = [times(left, (nh[t * width:(t + 1) * width, :], nl[t * width:(t + 1) * width, :])) for t in range(2)]
        here = slice(q * width, (q + 1) * width)
        uh[here, :], ul[here, :] = split(mixed(jnp.concatenate(theta, axis=1), gate, width))

    factor = newton_schulz(gram * inverse, [functools.partial(ahead, q) for q in range(2)])
    scale = math.sqrt(2 * width) * jnp.sqrt(inverse)
    for t in range(2):
        value = times((nh[t * width:(t + 1) * width, :], nl[t * width:(t + 1) * width, :]), factor) * scale
        bh[:, t * width:(t + 1) * width], bl[:, t * width:(t + 1) * width] = split(value)

    right = (bh[...], bl[...])
    squares = None
    for q in range(2):
        here = slice(q * width, (q + 1) * width)
        matrix = []
        for t in range(2):
            there = slice(t * width, (t + 1) * width)
            matrix.append(times((uh[here, there], ul[here, there]), factor) * scale)
        matrix = split(jnp.concatenate(matrix, axis=1))
        mh[here, :], ml[here, :] = matrix
        projected = times_transposed(matrix, right)
        square = sum_of_squares(projected)
        squares = square if squares is None else squares + square
        ph[:, here], pl_[:, here] = split(projected.T)
        piece = split(projected)
        for s in range(2):
            to = slice(s * width + q * half, s * width + (q + 1) * half)
            nh[to, :] = piece[0][s * half:(s + 1) * half]
            nl[to, :] = piece[1][s * half:(s + 1) * half]
    turned = (ph[...], pl_[...])
    inverse = 1.0 / (squares + EPSILON)
    gram = times_transposed(turned, turned) * inverse
    root = jnp.sqrt(inverse)

    def carry(q):
        here = slice(q * width, (q + 1) * width)
        kept[:, here] = times(turned, (mh[:, here], ml[:, here])) * root

    factor = newton_schulz(gram, [functools.partial(carry, q) for q in range(2)])

    outs = []

    def put(h):
        site = lax.rem(slab * 2 * RING + 2 * ring + 1 + h, 4 * chains)
        chain_to, slot = (site // 4, site % 4)
        for k in range(2):
            j = lax.rem(bond % RING // 2 + 1 + k, 2)
            bond_to = replica * RING + 2 * j + core
            src = obuf.at[h, pl.ds(bond_to * tall, tall)]
            dst = out_ref.at[pl.ds(slot * tall, tall)]
            copy = remote(src, dst, o_send.at[h, k], o_recv.at[slot], chain_to, bond_to)
            here = pltpu.make_async_copy(src, dst, o_recv.at[slot])
            mine = jnp.logical_and(chain_to == chain, bond_to == bond)
            outs.append((copy, mine))
            pl.when(mine)(here.start)
            pl.when(jnp.logical_not(mine))(copy.start)

    wanted = [(s, j) for j in range(2) for s in range(2)]
    picked = tuple(
        jnp.concatenate(
            [ref[pl.ds(s * width + (replica * RING + 2 * j + core) * rows, rows), :] for s, j in wanted], axis=0
        )
        for ref in (nh, nl)
    )
    value = times(picked, factor) * (math.sqrt(2 * width) * root)
    for k, (s, j) in enumerate(wanted):
        for t in range(2):
            at = (replica * RING + 2 * j + core) * tall + 2 * t + s
            obuf[0, pl.ds(at, rows, stride=4), :] = value[k * rows:(k + 1) * rows, t * LANES:(t + 1) * LANES]
    put(0)
    carried = times(factor, split(kept[...]))
    scale_norm = norm_of(carried)
    weight_odd = jnp.log(scale_norm)
    new_right = carried * (1.0 / scale_norm)

    row = lax.broadcasted_iota(jnp.int32, (8, LANES), 0)
    lane = lax.broadcasted_iota(jnp.int32, (8, LANES), 1)
    own = wall.at[slab * RING + ring]
    own[...] = jnp.where(row == 0, weight_even, weight_odd)
    weights = []
    for dz in range(slabs):
        for dk in range(RING):
            if dz == 0 and dk == 0:
                continue
            slab_at = lax.rem(slab + dz, slabs)
            bond_to = replica * RING + place_of(lax.rem(ring + dk, RING), slab_at)
            at = dz * RING + dk
            copy = remote(own, own, w_send.at[at], w_recv.at[at], 2 * slab_at + core, bond_to)
            copy.start()
            weights.append((copy, dz, dk))
    for s in range(2):
        for t in range(2):
            obuf[1, pl.ds(2 * t + s, width, stride=4), :] = new_right[:, s * width + t * LANES:s * width + (t + 1) * LANES]
    put(1)
    for copy, dz, dk in weights:
        source = lax.rem(slab + slabs - dz, slabs) * RING + lax.rem(ring + RING - dk, RING)
        landed(wall.at[source], w_recv.at[dz * RING + dk])
    total = jnp.zeros((8, LANES), jnp.float32)
    for e in range(slabs * RING):
        counted = jnp.logical_and(row < 2, 2 * e + row <= 4 * chain + lane)
        total = total + jnp.where(counted, wall[e], 0.0)
    running = jnp.sum(total, axis=0, keepdims=True) * (1.0 / (4 * chains))
    profile_ref[...] = jnp.broadcast_to(running, (8, LANES))

    for slot in range(4):
        landed(out_ref.at[pl.ds(slot * tall, tall)], o_recv.at[slot])
    for copy, mine in gathers:
        pl.when(jnp.logical_not(mine))(copy.wait_send)
    gate_copy.wait_send()
    for copy in forwards + passed + [c for c, dz, dk in weights]:
        copy.wait_send()
    for copy, mine in outs:
        pl.when(jnp.logical_not(mine))(copy.wait_send)


def per_device(chains, bonds, site_tensors, bond_gates):
    sites, rows, spins, width = site_tensors.shape
    assert sites == 4 and spins == 2 and width == 2 * LANES and bonds % RING == 0 and chains % 2 == 0
    cut = (sites, rows, spins, width // LANES, LANES)
    flat = site_tensors.reshape(cut).transpose(0, 1, 3, 2, 4).reshape(sites * rows * 4, LANES)
    slabs = chains // 2
    dma = pltpu.SemaphoreType.DMA
    wide, tall = ((width, 2 * width), (2 * width, width))
    half = [pltpu.VMEM(shape, jnp.bfloat16) for shape in (wide, wide, tall, tall, (2 * width, 2 * width), (2 * width, 2 * width), wide, wide, tall, tall, tall, tall, (2 * width, 2 * width), (2 * width, 2 * width))]
    out, profile = pl.pallas_call(
        functools.partial(kernel, chains, bonds, rows, width),
        out_shape=(
            jax.ShapeDtypeStruct(flat.shape, jnp.float32),
            jax.ShapeDtypeStruct((8, LANES), jnp.float32),
        ),
        in_specs=[pl.BlockSpec(memory_space=pltpu.HBM)] * 2,
        out_specs=(pl.BlockSpec(memory_space=pl.ANY), pl.BlockSpec(memory_space=pltpu.VMEM)),
        scratch_shapes=[
            pltpu.SemaphoreType.REGULAR,
            pltpu.SemaphoreType.REGULAR,
            dma,
            pltpu.VMEM(flat.shape, jnp.float32),
            pltpu.VMEM((2, 4 * width, LANES), jnp.float32),
            pltpu.VMEM((2,) + bond_gates.shape, jnp.float32),
            pltpu.VMEM((2, width, width), jnp.float32),
            pltpu.VMEM((2, width, width), jnp.float32),
            pltpu.VMEM((2, 4 * width, LANES), jnp.float32),
            pltpu.VMEM((slabs * RING, 8, LANES), jnp.float32),
            *half,
            pltpu.VMEM(wide, jnp.float32),
            dma((2, 2, 2, bonds // RING)), dma((2, bonds)),
            dma((2, bonds)), dma((2, bonds)),
            dma, dma((2,)),
            dma((GROUPS,)), dma((GROUPS,)),
            dma((GROUPS,)), dma((GROUPS,)),
            dma((2, 2)), dma((4,)),
            dma((slabs * RING,)), dma((slabs * RING,)),
        ],
        compiler_params=pltpu.CompilerParams(
            has_side_effects=True, collective_id=0, vmem_limit_bytes=56_000_000
        ),
    )(flat, bond_gates)
    cut = (sites, rows, width // LANES, spins, LANES)
    state = out.reshape(cut).transpose(0, 1, 3, 2, 4).reshape(site_tensors.shape)
    return (state, profile[0, :sites])


def solution(mesh):
    chains, bonds = (mesh.shape["chain"], mesh.shape["bond"])
    return jax.shard_map(
        functools.partial(per_device, chains, bonds),
        mesh=mesh,
        in_specs=(P("chain", "bond", None, None), P("chain", None, None)),
        out_specs=(P("chain", "bond", None, None), P("chain")),
        check_vma=False,
    )
```

```python
import functools
import math

import jax
import jax.numpy as jnp
from jax import lax
from jax.experimental import pallas as pl
from jax.experimental.pallas import tpu as pltpu
from jax.sharding import PartitionSpec as P

NS_ITERS = 3
RING = 4
GROUPS = 4
LANES = 128
EPSILON = 1e-06


def split(value):
    high = value.astype(jnp.bfloat16)
    low = (value - high.astype(jnp.float32)).astype(jnp.bfloat16)
    return (high, low)


def dot(a, b):
    return jnp.dot(a, b, preferred_element_type=jnp.float32)


def dot_t(a, b):
    return lax.dot_general(a, b, (((1,), (1,)), ((), ())), preferred_element_type=jnp.float32)


def times(a, b):
    (ah, al), (bh, bl) = (a, b)
    return dot(ah, bh) + dot(al, bh) + dot(ah, bl)


def times_transposed(a, b):
    (ah, al), (bh, bl) = (a, b)
    return dot_t(ah, bh) + dot_t(al, bh) + dot_t(ah, bl)


def mixed(theta, gate, width):
    r = theta.shape[0] // 2
    theta = [[theta[u * r:(u + 1) * r, v * width:(v + 1) * width] for v in range(2)] for u in range(2)]
    scaled = gate * (1.0 / math.sqrt(width))
    rows = []
    for s in range(2):
        row = []
        for t in range(2):
            total = None
            for u in range(2):
                for v in range(2):
                    factor = scaled[2 * s + t:2 * s + t + 1, 2 * u + v:2 * u + v + 1]
                    term = factor * theta[u][v]
                    total = term if total is None else total + term
            row.append(total)
        rows.append(jnp.concatenate(row, axis=1))
    return jnp.concatenate(rows, axis=0)


def newton_schulz(gram, fill=()):
    assert NS_ITERS == 3
    fill = list(fill)

    def filled(value):
        if fill:
            fill.pop(0)()
        return value

    eye = jnp.where(
        lax.broadcasted_iota(jnp.int32, gram.shape, 0) == lax.broadcasted_iota(jnp.int32, gram.shape, 1),
        jnp.float32(1.5),
        jnp.float32(0.0),
    )
    factor = None
    for repeat in range(NS_ITERS):
        step = eye - 0.5 * gram
        factor = step if factor is None else times(split(factor), split(step))
        if repeat < NS_ITERS - 1:
            gram_split = split(gram)
            once = 1.5 * gram - 0.5 * filled(times(gram_split, gram_split))
            gram = 1.5 * once - 0.5 * filled(times(split(once), gram_split))
    while fill:
        fill.pop(0)()
    return split(factor)


def sum_of_squares(value):
    return jnp.sum(value * value, keepdims=True)


def norm_of(carried):
    mean = sum_of_squares(carried) * (1.0 / carried.size)
    return jnp.sqrt(mean + EPSILON)


def order(place):
    return place + (place // 2) * (1 - 2 * (place % 2))


def grouped(mine, d):
    if d == 0:
        return mine
    if d == 1:
        return mine + 1 - 2 * (mine % 2)
    if d == 2:
        return lax.rem(mine + 2, 4)
    return 3 - mine


def kernel(
    chains, bonds, rows, width,
    x_ref, gates_ref, out_ref, profile_ref,
    slab_sem, ring_sem, fetch_sem, xin, inbuf, gates, rsend, rrecv, obuf, wall, below,
    bh, bl, th, tl, mh, ml, ph, pl_, lh, ll, nh, nl, uh, ul, kept,
    g_send, g_recv, gate_send, gate_recv,
    m_send, m_recv, o_send, o_recv, w_send, w_recv, p_send, p_recv,
):
    chain, bond = (lax.axis_index("chain"), lax.axis_index("bond"))
    slabs = chains // 2
    slab, core = (chain // 2, chain % 2)
    tall = rows * 4
    part = bonds // GROUPS
    tier = width // GROUPS
    half = width // 2
    replica = bond // RING
    ring = order(bond % RING)
    block = ring // 2

    def on(which):
        return pl.when(core == which)

    def at(slab_at, core_at, bond_at):
        return {"chain": 2 * slab_at + core_at, "bond": bond_at}

    def remote(src, dst, send, recv_sem, to):
        return pltpu.make_async_remote_copy(
            src_ref=src, dst_ref=dst, send_sem=send, recv_sem=recv_sem,
            device_id=to, device_id_type=pl.DeviceIdType.MESH,
        )

    def landed(ref, sem):
        pltpu.make_async_copy(ref, ref, sem).wait()

    def greet(semaphore, to):
        pl.semaphore_signal(semaphore, inc=1, device_id=to, device_id_type=pl.DeviceIdType.MESH)

    fetch = pltpu.make_async_copy(x_ref, xin, fetch_sem)
    fetch.start()
    gate_here = pltpu.make_async_copy(gates_ref, gates.at[1], gate_recv.at[1])
    gate_copy = remote(gates_ref, gates.at[0], gate_send, gate_recv.at[0], at(slab, 1, bond))
    barrier = pltpu.get_barrier_semaphore()

    @on(1)
    def _():
        gate_here.start()
        for db in range(1, bonds):
            greet(barrier, at(slab, 1, lax.rem(bond + db, bonds)))

    @on(0)
    def _():
        greet(barrier, at(slab, 1, bond))
        for db in range(1, RING):
            greet(barrier, at(slab, 0, replica * RING + lax.rem(bond + db, RING)))

    for dz in range(1, slabs):
        for db in range(RING):
            greet(barrier, at(lax.rem(slab + dz, slabs), 0, replica * RING + lax.rem(bond + db, RING)))

    @on(1)
    def _():
        pl.semaphore_wait(barrier, bonds)
        greet(slab_sem, at(slab, 0, bond))

    @on(0)
    def _():
        pl.semaphore_wait(slab_sem, 1)

    fetch.wait()
    gathers = []
    for i in (1, 0):
        for j in range(2):
            for r in range(bonds // RING):
                bond_to = r * RING + order(2 * core + j)
                src = xin.at[pl.ds((2 * j + i) * tall, tall)]
                dst = inbuf.at[i, pl.ds(bond * tall, tall)]
                sem = g_recv.at[i, bond]
                copy = remote(src, dst, g_send.at[i, j, r], sem, at(slab, 1, bond_to))
                here = pltpu.make_async_copy(src, dst, sem)
                mine = jnp.logical_and(core == 1, bond_to == bond)
                gathers.append((copy, here, mine))
                pl.when(jnp.logical_not(mine))(copy.start)
    for copy, here, mine in gathers:
        pl.when(mine)(here.start)

    def gathers_sent():
        for copy, here, mine in gathers:
            pl.when(jnp.logical_not(mine))(copy.wait_send)

    def outputs_landed():
        for slot in range(4):
            landed(out_ref.at[pl.ds(slot * tall, tall)], o_recv.at[slot])

    @on(0)
    def _():
        gate_copy.start()
        pl.semaphore_wait(barrier, RING - 1 + (slabs - 1) * 2 * RING)
        greet(ring_sem, at(slab, 1, bond))
        gathers_sent()
        gate_copy.wait_send()
        outputs_landed()
        landed(profile_ref, p_recv)

    def gathered(i, d):
        for e in range(part):
            origin = grouped(bond // part, d) * part + lax.rem(bond + e, part)
            landed(inbuf.at[i, pl.ds(origin * tall, tall)], g_recv.at[i, origin])

    def spin(i, s, row, count):
        return jnp.concatenate(
            [inbuf[i, pl.ds(4 * row + 2 * t + s, count, stride=4), :] for t in range(2)], axis=1
        )

    @on(1)
    def _():
        before = lax.rem(ring + RING - 1, RING)
        slab_to = lax.rem(slab + slabs - jnp.where(ring == 0, 1, 0), slabs)
        previous = at(slab_to, 1, replica * RING + order(before))
        next_bond = replica * RING + order(lax.rem(ring + 1, RING))

        for d in range(GROUPS):
            gathered(1, d)
        landed(gates.at[0], gate_recv.at[0])
        landed(gates.at[1], gate_recv.at[1])
        right = jnp.concatenate([spin(1, s, 0, width) for s in range(2)], axis=1)
        bh[...], bl[...] = split(right)
        th[...], tl[...] = split(right.T)
        pl.semaphore_wait(ring_sem, 1)

        gate = gates[block, 2 * (ring % 2)]
        passed = []
        squares = None
        for d in range(GROUPS):
            g = grouped(bond // part, d)
            gathered(0, d)
            left = jnp.concatenate([spin(0, s, g * tier, tier) for s in range(2)], axis=0)
            theta = times(split(left), (bh[...], bl[...]))
            matrix = split(mixed(theta, gate, width))
            here = pl.ds(d * 2 * tier, 2 * tier)
            mh[here, :], ml[here, :] = matrix
            projected = times(matrix, (th[...], tl[...]))
            piece = pl.ds(g * 2 * tier, 2 * tier)
            rsend[piece, :] = projected
            copy = remote(rsend.at[piece], rrecv.at[piece], m_send.at[d], m_recv.at[d], previous)
            copy.start()
            passed.append(copy)
            square = sum_of_squares(projected)
            squares = square if squares is None else squares + square
            ph[:, here], pl_[:, here] = split(projected.T)

        turned = (ph[...], pl_[...])
        inverse = 1.0 / (squares + EPSILON)
        gram = times_transposed(turned, turned) * inverse
        root = jnp.sqrt(inverse)

        def carry_even(q):
            here = slice(q * width, (q + 1) * width)
            kept[:, here] = times(turned, (mh[:, here], ml[:, here])) * root

        factor = newton_schulz(gram, [functools.partial(carry_even, q) for q in range(2)])
        carried = times(factor, split(kept[...]))
        scale_norm = norm_of(carried)
        weight_even = jnp.log(scale_norm)
        carried = split(carried * (1.0 / scale_norm))
        for s in range(2):
            lh[s * width:(s + 1) * width, :] = carried[0][:, s * width:(s + 1) * width]
            ll[s * width:(s + 1) * width, :] = carried[1][:, s * width:(s + 1) * width]

        gram = None
        squares = None
        for d in range(1, GROUPS, 2):
            parts = []
            for e in (d - 1, d):
                g = grouped(next_bond // part, e)
                piece = pl.ds(g * 2 * tier, 2 * tier)
                landed(rrecv.at[piece], m_recv.at[e])
                parts.append(rrecv[piece, :])
            received = jnp.concatenate(parts, axis=0)
            square = sum_of_squares(received)
            squares = square if squares is None else squares + square
            turned = split(received.T)
            piece = split(received)
            for k, (e, s) in enumerate([(e, s) for e in (d - 1, d) for s in range(2)]):
                g = grouped(next_bond // part, e)
                nh[pl.ds(s * width + g * tier, tier), :] = piece[0][k * tier:(k + 1) * tier]
                nl[pl.ds(s * width + g * tier, tier), :] = piece[1][k * tier:(k + 1) * tier]
            product = times(turned, piece)
            gram = product if gram is None else gram + product
        inverse = 1.0 / (squares + EPSILON)
        gate = gates[block, 2 * (ring % 2) + 1]

        def ahead(q):
            left = tuple(
                jnp.concatenate([ref[s * width + q * half:s * width + (q + 1) * half, :] for s in range(2)], axis=0)
                for ref in (lh, ll)
            )
            theta = [times(left, (nh[t * width:(t + 1) * width, :], nl[t * width:(t + 1) * width, :])) for t in range(2)]
            here = slice(q * width, (q + 1) * width)
            uh[here, :], ul[here, :] = split(mixed(jnp.concatenate(theta, axis=1), gate, width))

        factor = newton_schulz(gram * inverse, [functools.partial(ahead, q) for q in range(2)])
        scale = math.sqrt(2 * width) * jnp.sqrt(inverse)
        for t in range(2):
            value = times((nh[t * width:(t + 1) * width, :], nl[t * width:(t + 1) * width, :]), factor) * scale
            bh[:, t * width:(t + 1) * width], bl[:, t * width:(t + 1) * width] = split(value)

        right = (bh[...], bl[...])
        squares = None
        for q in range(2):
            here = slice(q * width, (q + 1) * width)
            matrix = []
            for t in range(2):
                there = slice(t * width, (t + 1) * width)
                matrix.append(times((uh[here, there], ul[here, there]), factor) * scale)
            matrix = split(jnp.concatenate(matrix, axis=1))
            mh[here, :], ml[here, :] = matrix
            projected = times_transposed(matrix, right)
            square = sum_of_squares(projected)
            squares = square if squares is None else squares + square
            ph[:, here], pl_[:, here] = split(projected.T)
            piece = split(projected)
            for s in range(2):
                to = slice(s * width + q * half, s * width + (q + 1) * half)
                nh[to, :] = piece[0][s * half:(s + 1) * half]
                nl[to, :] = piece[1][s * half:(s + 1) * half]
        turned = (ph[...], pl_[...])
        inverse = 1.0 / (squares + EPSILON)
        gram = times_transposed(turned, turned) * inverse
        root = jnp.sqrt(inverse)

        def carry(q):
            here = slice(q * width, (q + 1) * width)
            kept[:, here] = times(turned, (mh[:, here], ml[:, here])) * root

        factor = newton_schulz(gram, [functools.partial(carry, q) for q in range(2)])
        outs = []

        def put(h):
            site = lax.rem(slab * 2 * RING + 2 * ring + 1 + h, 4 * chains)
            chain_to, slot = (site // 4, site % 4)
            for k in range(RING):
                bond_to = replica * RING + grouped(bond % RING, RING - 1 - k)
                src = obuf.at[h, pl.ds(bond_to * tall, tall)]
                dst = out_ref.at[pl.ds(slot * tall, tall)]
                copy = remote(src, dst, o_send.at[h, k], o_recv.at[slot], {"chain": chain_to, "bond": bond_to})
                if k < RING - 1:
                    copy.start()
                    outs.append((copy, None))
                    continue
                here = pltpu.make_async_copy(src, dst, o_recv.at[slot])
                mine = chain_to == chain
                outs.append((copy, mine))
                pl.when(mine)(here.start)
                pl.when(jnp.logical_not(mine))(copy.start)

        carried = times(factor, split(kept[...]))
        scale_norm = norm_of(carried)
        weight_odd = jnp.log(scale_norm)
        new_right = carried * (1.0 / scale_norm)

        row = lax.broadcasted_iota(jnp.int32, (8, LANES), 0)
        lane = lax.broadcasted_iota(jnp.int32, (8, LANES), 1)
        own = wall.at[slab * RING + ring]
        own[...] = jnp.where(row == 0, weight_even, weight_odd)
        weights = []
        for dz in range(slabs):
            for dk in range(RING):
                if dz == 0 and dk == 0:
                    continue
                to = at(lax.rem(slab + dz, slabs), 1, replica * RING + order(lax.rem(ring + dk, RING)))
                k = dz * RING + dk
                copy = remote(own, own, w_send.at[k], w_recv.at[k], to)
                copy.start()
                weights.append((copy, dz, dk))
        for s in range(2):
            for t in range(2):
                obuf[1, pl.ds(2 * t + s, width, stride=4), :] = (
                    new_right[:, s * width + t * LANES:s * width + (t + 1) * LANES]
                )
        put(1)
        value = times((nh[...], nl[...]), factor) * (math.sqrt(2 * width) * root)
        for s in range(2):
            for t in range(2):
                obuf[0, pl.ds(2 * t + s, width, stride=4), :] = (
                    value[s * width:(s + 1) * width, t * LANES:(t + 1) * LANES]
                )
        put(0)

        for copy, dz, dk in weights:
            source = lax.rem(slab + slabs - dz, slabs) * RING + lax.rem(ring + RING - dk, RING)
            landed(wall.at[source], w_recv.at[dz * RING + dk])
        totals = [jnp.zeros((8, LANES), jnp.float32) for _ in range(2)]
        for e in range(slabs * RING):
            for c in range(2):
                counted = jnp.logical_and(row < 2, 2 * e + row <= 4 * (2 * slab + c) + lane)
                totals[c] = totals[c] + jnp.where(counted, wall[e], 0.0)
        running = [
            jnp.broadcast_to(jnp.sum(total, axis=0, keepdims=True) * (1.0 / (4 * chains)), (8, LANES))
            for total in totals
        ]
        below[...] = running[0]
        profile_ref[...] = running[1]
        lower = remote(below, profile_ref, p_send, p_recv, at(slab, 0, bond))
        lower.start()

        outputs_landed()
        gathers_sent()
        for copy in passed + [c for c, dz, dk in weights] + [lower]:
            copy.wait_send()
        for copy, mine in outs:
            if mine is None:
                copy.wait_send()
            else:
                pl.when(jnp.logical_not(mine))(copy.wait_send)


def per_device(chains, bonds, site_tensors, bond_gates):
    sites, rows, spins, width = site_tensors.shape
    assert sites == 4 and spins == 2 and width == 2 * LANES and bonds % RING == 0 and chains % 2 == 0
    cut = (sites, rows, spins, width // LANES, LANES)
    flat = site_tensors.reshape(cut).transpose(0, 1, 3, 2, 4).reshape(sites * rows * 4, LANES)
    slabs = chains // 2
    dma = pltpu.SemaphoreType.DMA
    wide, tall = ((width, 2 * width), (2 * width, width))
    half = [pltpu.VMEM(shape, jnp.bfloat16) for shape in (wide, wide, tall, tall, (2 * width, 2 * width), (2 * width, 2 * width), wide, wide, tall, tall, tall, tall, (2 * width, 2 * width), (2 * width, 2 * width))]
    out, profile = pl.pallas_call(
        functools.partial(kernel, chains, bonds, rows, width),
        out_shape=(
            jax.ShapeDtypeStruct(flat.shape, jnp.float32),
            jax.ShapeDtypeStruct((8, LANES), jnp.float32),
        ),
        in_specs=[pl.BlockSpec(memory_space=pltpu.HBM)] * 2,
        out_specs=(pl.BlockSpec(memory_space=pl.ANY), pl.BlockSpec(memory_space=pltpu.VMEM)),
        scratch_shapes=[
            pltpu.SemaphoreType.REGULAR,
            pltpu.SemaphoreType.REGULAR,
            dma,
            pltpu.VMEM(flat.shape, jnp.float32),
            pltpu.VMEM((2, 4 * width, LANES), jnp.float32),
            pltpu.VMEM((2,) + bond_gates.shape, jnp.float32),
            pltpu.VMEM((2 * width, width), jnp.float32),
            pltpu.VMEM((2 * width, width), jnp.float32),
            pltpu.VMEM((2, 4 * width, LANES), jnp.float32),
            pltpu.VMEM((slabs * RING, 8, LANES), jnp.float32),
            pltpu.VMEM((8, LANES), jnp.float32),
            *half,
            pltpu.VMEM(wide, jnp.float32),
            dma((2, 2, bonds // RING)), dma((2, bonds)),
            dma, dma((2,)),
            dma((GROUPS,)), dma((GROUPS,)),
            dma((2, RING)), dma((4,)),
            dma((slabs * RING,)), dma((slabs * RING,)),
            dma, dma,
        ],
        compiler_params=pltpu.CompilerParams(
            has_side_effects=True, collective_id=0, vmem_limit_bytes=56_000_000
        ),
    )(flat, bond_gates)
    cut = (sites, rows, width // LANES, spins, LANES)
    state = out.reshape(cut).transpose(0, 1, 3, 2, 4).reshape(site_tensors.shape)
    return (state, profile[0, :sites])


def solution(mesh):
    chains, bonds = (mesh.shape["chain"], mesh.shape["bond"])
    return jax.shard_map(
        functools.partial(per_device, chains, bonds),
        mesh=mesh,
        in_specs=(P("chain", "bond", None, None), P("chain", None, None)),
        out_specs=(P("chain", "bond", None, None), P("chain")),
        check_vma=False,
    )
```

```python
import functools
import math

import jax
import jax.numpy as jnp
from jax import lax
from jax.experimental import pallas as pl
from jax.experimental.pallas import tpu as pltpu
from jax.sharding import PartitionSpec as P

NS_ITERS = 3
RING = 4
GROUPS = 4
PIECES = 1
LANES = 128
EPSILON = 1e-06


def split(value):
    high = value.astype(jnp.bfloat16)
    low = (value - high.astype(jnp.float32)).astype(jnp.bfloat16)
    return (high, low)


def dot(a, b):
    return jnp.dot(a, b, preferred_element_type=jnp.float32)


def dot_t(a, b):
    return lax.dot_general(a, b, (((1,), (1,)), ((), ())), preferred_element_type=jnp.float32)


def times(a, b):
    (ah, al), (bh, bl) = (a, b)
    return dot(ah, bh) + dot(al, bh) + dot(ah, bl)


def times_transposed(a, b):
    (ah, al), (bh, bl) = (a, b)
    return dot_t(ah, bh) + dot_t(al, bh) + dot_t(ah, bl)


def mixed(theta, gate, width):
    r = theta.shape[0] // 2
    theta = [[theta[u * r:(u + 1) * r, v * width:(v + 1) * width] for v in range(2)] for u in range(2)]
    scaled = gate * (1.0 / math.sqrt(width))
    rows = []
    for s in range(2):
        row = []
        for t in range(2):
            total = None
            for u in range(2):
                for v in range(2):
                    factor = scaled[2 * s + t:2 * s + t + 1, 2 * u + v:2 * u + v + 1]
                    term = factor * theta[u][v]
                    total = term if total is None else total + term
            row.append(total)
        rows.append(jnp.concatenate(row, axis=1))
    return jnp.concatenate(rows, axis=0)


def newton_schulz(gram, fill=()):
    assert NS_ITERS == 3
    fill = list(fill)

    def filled(value):
        if fill:
            fill.pop(0)()
        return value

    eye = jnp.where(
        lax.broadcasted_iota(jnp.int32, gram.shape, 0) == lax.broadcasted_iota(jnp.int32, gram.shape, 1),
        jnp.float32(1.5),
        jnp.float32(0.0),
    )
    factor = None
    for repeat in range(NS_ITERS):
        step = eye - 0.5 * gram
        factor = step if factor is None else times(split(factor), split(step))
        if repeat < NS_ITERS - 1:
            gram_split = split(gram)
            once = 1.5 * gram - 0.5 * filled(times(gram_split, gram_split))
            gram = 1.5 * once - 0.5 * filled(times(split(once), gram_split))
    while fill:
        fill.pop(0)()
    return split(factor)


def sum_of_squares(value):
    return jnp.sum(value * value, keepdims=True)


def norm_of(carried):
    mean = sum_of_squares(carried) * (1.0 / carried.size)
    return jnp.sqrt(mean + EPSILON)


def order(place):
    return place + (place // 2) * (1 - 2 * (place % 2))


def grouped(mine, d):
    if d == 0:
        return mine
    if d == 1:
        return mine + 1 - 2 * (mine % 2)
    if d == 2:
        return lax.rem(mine + 2, 4)
    return 3 - mine


def kernel(
    chains, bonds, rows, width,
    x_ref, gates_ref, out_ref, profile_ref,
    slab_sem, ring_sem, fetch_sem, xin, inbuf, gates, rsend, rrecv, obuf, wall, below,
    bh, bl, th, tl, mh, ml, ph, pl_, lh, ll, nh, nl, uh, ul, kept,
    g_send, g_recv, gate_send, gate_recv,
    m_send, m_recv, o_send, o_recv, w_send, w_recv, p_send, p_recv,
):
    chain, bond = (lax.axis_index("chain"), lax.axis_index("bond"))
    slabs = chains // 2
    slab, core = (chain // 2, chain % 2)
    tall = rows * 4
    part = bonds // GROUPS
    tier = width // GROUPS
    half = width // 2
    replica = bond // RING
    ring = order(bond % RING)
    block = ring // 2

    def on(which):
        return pl.when(core == which)

    def at(slab_at, core_at, bond_at):
        return {"chain": 2 * slab_at + core_at, "bond": bond_at}

    def remote(src, dst, send, recv_sem, to):
        return pltpu.make_async_remote_copy(
            src_ref=src, dst_ref=dst, send_sem=send, recv_sem=recv_sem,
            device_id=to, device_id_type=pl.DeviceIdType.MESH,
        )

    def landed(ref, sem):
        pltpu.make_async_copy(ref, ref, sem).wait()

    def greet(semaphore, to):
        pl.semaphore_signal(semaphore, inc=1, device_id=to, device_id_type=pl.DeviceIdType.MESH)

    fetch = pltpu.make_async_copy(x_ref, xin, fetch_sem)
    fetch.start()
    gate_here = pltpu.make_async_copy(gates_ref, gates.at[1], gate_recv.at[1])
    gate_copy = remote(gates_ref, gates.at[0], gate_send, gate_recv.at[0], at(slab, 1, bond))
    barrier = pltpu.get_barrier_semaphore()

    @on(1)
    def _():
        gate_here.start()
        for db in range(1, bonds):
            greet(barrier, at(slab, 1, lax.rem(bond + db, bonds)))

    @on(0)
    def _():
        greet(barrier, at(slab, 1, bond))
        for db in range(1, RING):
            greet(barrier, at(slab, 0, replica * RING + lax.rem(bond + db, RING)))

    for dz in range(1, slabs):
        for db in range(RING):
            greet(barrier, at(lax.rem(slab + dz, slabs), 0, replica * RING + lax.rem(bond + db, RING)))

    @on(1)
    def _():
        pl.semaphore_wait(barrier, bonds)
        greet(slab_sem, at(slab, 0, bond))

    @on(0)
    def _():
        pl.semaphore_wait(slab_sem, 1)

    fetch.wait()
    gathers = []
    for i in (1, 0):
        for j in range(2):
            for r in range(bonds // RING):
                bond_to = r * RING + order(2 * core + j)
                src = xin.at[pl.ds((2 * j + i) * tall, tall)]
                dst = inbuf.at[i, pl.ds(bond * tall, tall)]
                sem = g_recv.at[i, bond]
                copy = remote(src, dst, g_send.at[i, j, r], sem, at(slab, 1, bond_to))
                here = pltpu.make_async_copy(src, dst, sem)
                mine = jnp.logical_and(core == 1, bond_to == bond)
                gathers.append((copy, here, mine))
                pl.when(jnp.logical_not(mine))(copy.start)
    for copy, here, mine in gathers:
        pl.when(mine)(here.start)

    def gathers_sent():
        for copy, here, mine in gathers:
            pl.when(jnp.logical_not(mine))(copy.wait_send)

    def outputs_landed():
        for slot in range(4):
            landed(out_ref.at[pl.ds(slot * tall, tall)], o_recv.at[slot])

    @on(0)
    def _():
        gate_copy.start()
        pl.semaphore_wait(barrier, RING - 1 + (slabs - 1) * 2 * RING)
        greet(ring_sem, at(slab, 1, bond))
        gathers_sent()
        gate_copy.wait_send()
        outputs_landed()
        landed(profile_ref, p_recv)

    def gathered(i, d):
        for e in range(part):
            origin = grouped(bond // part, d) * part + lax.rem(bond + e, part)
            landed(inbuf.at[i, pl.ds(origin * tall, tall)], g_recv.at[i, origin])

    def spin(i, s, row, count):
        return jnp.concatenate(
            [inbuf[i, pl.ds(4 * row + 2 * t + s, count, stride=4), :] for t in range(2)], axis=1
        )

    @on(1)
    def _():
        before = lax.rem(ring + RING - 1, RING)
        slab_to = lax.rem(slab + slabs - jnp.where(ring == 0, 1, 0), slabs)
        previous = at(slab_to, 1, replica * RING + order(before))
        next_bond = replica * RING + order(lax.rem(ring + 1, RING))

        for d in range(GROUPS):
            gathered(1, d)
        landed(gates.at[0], gate_recv.at[0])
        landed(gates.at[1], gate_recv.at[1])
        right = jnp.concatenate([spin(1, s, 0, width) for s in range(2)], axis=1)
        bh[...], bl[...] = split(right)
        th[...], tl[...] = split(right.T)
        pl.semaphore_wait(ring_sem, 1)

        gate = gates[block, 2 * (ring % 2)]
        passed = []
        squares = None
        for d in range(GROUPS):
            g = grouped(bond // part, d)
            gathered(0, d)
            left = jnp.concatenate([spin(0, s, g * tier, tier) for s in range(2)], axis=0)
            theta = times(split(left), (bh[...], bl[...]))
            matrix = split(mixed(theta, gate, width))
            here = pl.ds(d * 2 * tier, 2 * tier)
            mh[here, :], ml[here, :] = matrix
            projected = times(matrix, (th[...], tl[...]))
            piece = pl.ds(g * 2 * tier, 2 * tier)
            rsend[piece, :] = projected
            copy = remote(rsend.at[piece], rrecv.at[piece], m_send.at[d], m_recv.at[d], previous)
            copy.start()
            passed.append(copy)
            square = sum_of_squares(projected)
            squares = square if squares is None else squares + square
            ph[:, here], pl_[:, here] = split(projected.T)

        turned = (ph[...], pl_[...])
        inverse = 1.0 / (squares + EPSILON)
        gram = times_transposed(turned, turned) * inverse
        root = jnp.sqrt(inverse)

        def carry_even(q):
            here = slice(q * width, (q + 1) * width)
            kept[:, here] = times(turned, (mh[:, here], ml[:, here])) * root

        factor = newton_schulz(gram, [functools.partial(carry_even, q) for q in range(2)])
        carried = times(factor, split(kept[...]))
        scale_norm = norm_of(carried)
        weight_even = jnp.log(scale_norm)
        carried = split(carried * (1.0 / scale_norm))
        for s in range(2):
            lh[s * width:(s + 1) * width, :] = carried[0][:, s * width:(s + 1) * width]
            ll[s * width:(s + 1) * width, :] = carried[1][:, s * width:(s + 1) * width]

        gram = None
        squares = None
        for d in range(1, GROUPS, 2):
            parts = []
            for e in (d - 1, d):
                g = grouped(next_bond // part, e)
                piece = pl.ds(g * 2 * tier, 2 * tier)
                landed(rrecv.at[piece], m_recv.at[e])
                parts.append(rrecv[piece, :])
            received = jnp.concatenate(parts, axis=0)
            square = sum_of_squares(received)
            squares = square if squares is None else squares + square
            turned = split(received.T)
            piece = split(received)
            for k, (e, s) in enumerate([(e, s) for e in (d - 1, d) for s in range(2)]):
                g = grouped(next_bond // part, e)
                nh[pl.ds(s * width + g * tier, tier), :] = piece[0][k * tier:(k + 1) * tier]
                nl[pl.ds(s * width + g * tier, tier), :] = piece[1][k * tier:(k + 1) * tier]
            product = times(turned, piece)
            gram = product if gram is None else gram + product
        inverse = 1.0 / (squares + EPSILON)
        gate = gates[block, 2 * (ring % 2) + 1]

        def ahead(q):
            left = tuple(
                jnp.concatenate([ref[s * width + q * half:s * width + (q + 1) * half, :] for s in range(2)], axis=0)
                for ref in (lh, ll)
            )
            theta = [times(left, (nh[t * width:(t + 1) * width, :], nl[t * width:(t + 1) * width, :])) for t in range(2)]
            here = slice(q * width, (q + 1) * width)
            uh[here, :], ul[here, :] = split(mixed(jnp.concatenate(theta, axis=1), gate, width))

        factor = newton_schulz(gram * inverse, [functools.partial(ahead, q) for q in range(2)])
        scale = math.sqrt(2 * width) * jnp.sqrt(inverse)
        for t in range(2):
            value = times((nh[t * width:(t + 1) * width, :], nl[t * width:(t + 1) * width, :]), factor) * scale
            bh[:, t * width:(t + 1) * width], bl[:, t * width:(t + 1) * width] = split(value)

        right = (bh[...], bl[...])
        squares = None
        for q in range(2):
            here = slice(q * width, (q + 1) * width)
            matrix = []
            for t in range(2):
                there = slice(t * width, (t + 1) * width)
                matrix.append(times((uh[here, there], ul[here, there]), factor) * scale)
            matrix = split(jnp.concatenate(matrix, axis=1))
            mh[here, :], ml[here, :] = matrix
            projected = times_transposed(matrix, right)
            square = sum_of_squares(projected)
            squares = square if squares is None else squares + square
            ph[:, here], pl_[:, here] = split(projected.T)
            piece = split(projected)
            for s in range(2):
                to = slice(s * width + q * half, s * width + (q + 1) * half)
                nh[to, :] = piece[0][s * half:(s + 1) * half]
                nl[to, :] = piece[1][s * half:(s + 1) * half]
        turned = (ph[...], pl_[...])
        inverse = 1.0 / (squares + EPSILON)
        gram = times_transposed(turned, turned) * inverse
        root = jnp.sqrt(inverse)

        def carry(q):
            here = slice(q * width, (q + 1) * width)
            kept[:, here] = times(turned, (mh[:, here], ml[:, here])) * root

        factor = newton_schulz(gram, [functools.partial(carry, q) for q in range(2)])
        outs = []

        def put(h):
            site = lax.rem(slab * 2 * RING + 2 * ring + 1 + h, 4 * chains)
            chain_to, slot = (site // 4, site % 4)
            for k in range(RING):
                bond_to = replica * RING + grouped(bond % RING, RING - 1 - k)
                src = obuf.at[h, pl.ds(bond_to * tall, tall)]
                dst = out_ref.at[pl.ds(slot * tall, tall)]
                copy = remote(src, dst, o_send.at[h, k], o_recv.at[slot], {"chain": chain_to, "bond": bond_to})
                if k < RING - 1:
                    copy.start()
                    outs.append((copy, None))
                    continue
                here = pltpu.make_async_copy(src, dst, o_recv.at[slot])
                mine = chain_to == chain
                outs.append((copy, mine))
                pl.when(mine)(here.start)
                pl.when(jnp.logical_not(mine))(copy.start)

        carried = times(factor, split(kept[...]))
        scale_norm = norm_of(carried)
        weight_odd = jnp.log(scale_norm)
        new_right = carried * (1.0 / scale_norm)

        lane = lax.broadcasted_iota(jnp.int32, (1, LANES), 1)
        odd = lane // (LANES // 2)
        own = wall.at[slab * RING + ring]
        own[...] = jnp.where(odd == 0, weight_even, weight_odd)
        weights = []
        for dz in range(slabs):
            for dk in range(RING):
                if dz == 0 and dk == 0:
                    continue
                to = at(lax.rem(slab + dz, slabs), 1, replica * RING + order(lax.rem(ring + dk, RING)))
                k = dz * RING + dk
                copy = remote(own, own, w_send.at[k], w_recv.at[k], to)
                pl.when(slab + dz < slabs)(copy.start)
                weights.append((copy, dz, dk))
        for s in range(2):
            for t in range(2):
                obuf[1, pl.ds(2 * t + s, width, stride=4), :] = (
                    new_right[:, s * width + t * LANES:s * width + (t + 1) * LANES]
                )
        put(1)
        value = times((nh[...], nl[...]), factor) * (math.sqrt(2 * width) * root)
        for s in range(2):
            for t in range(2):
                obuf[0, pl.ds(2 * t + s, width, stride=4), :] = (
                    value[s * width:(s + 1) * width, t * LANES:(t + 1) * LANES]
                )
        put(0)

        for copy, dz, dk in weights:
            source = lax.rem(slab + slabs - dz, slabs) * RING + lax.rem(ring + RING - dk, RING)

            @pl.when(slab >= dz)
            def _():
                landed(wall.at[source], w_recv.at[dz * RING + dk])
        totals = [jnp.zeros((1, LANES), jnp.float32) for _ in range(2)]
        for e in range(slabs * RING):
            for c in range(2):
                counted = 2 * e + odd <= 4 * (2 * slab + c) + lane % (LANES // 2)
                totals[c] = totals[c] + jnp.where(counted, wall[e], 0.0)
        running = [
            jnp.broadcast_to((total + pltpu.roll(total, LANES // 2, 1)) * (1.0 / (4 * chains)), (8, LANES))
            for total in totals
        ]
        below[...] = running[0]
        profile_ref[...] = running[1]
        lower = remote(below, profile_ref, p_send, p_recv, at(slab, 0, bond))
        lower.start()

        outputs_landed()
        gathers_sent()
        for copy in passed + [lower]:
            copy.wait_send()
        for copy, dz, dk in weights:
            pl.when(slab + dz < slabs)(copy.wait_send)
        for copy, mine in outs:
            if mine is None:
                copy.wait_send()
            else:
                pl.when(jnp.logical_not(mine))(copy.wait_send)


def finish(out_ref, weights_ref, state_ref, profile_ref, held, state_sem, profile_sem):
    held[...] = weights_ref[0, :held.shape[0]]
    last = pltpu.make_async_copy(held, profile_ref, profile_sem)
    last.start()
    size = out_ref.shape[0] // PIECES
    copies = []
    for k in range(PIECES):
        here = pl.ds(k * size, size)
        copy = pltpu.make_async_copy(out_ref.at[here], state_ref.at[here], state_sem.at[k])
        copy.start()
        copies.append(copy)
    for copy in copies:
        copy.wait()
    last.wait()


def per_device(chains, bonds, site_tensors, bond_gates):
    sites, rows, spins, width = site_tensors.shape
    assert sites == 4 and spins == 2 and width == 2 * LANES and bonds % RING == 0 and chains % 2 == 0
    cut = (sites, rows, spins, width // LANES, LANES)
    flat = site_tensors.reshape(cut).transpose(0, 1, 3, 2, 4).reshape(sites * rows * 4, LANES)
    slabs = chains // 2
    dma = pltpu.SemaphoreType.DMA
    wide, tall = ((width, 2 * width), (2 * width, width))
    half = [pltpu.VMEM(shape, jnp.bfloat16) for shape in (wide, wide, tall, tall, (2 * width, 2 * width), (2 * width, 2 * width), wide, wide, tall, tall, tall, tall, (2 * width, 2 * width), (2 * width, 2 * width))]
    out, profile = pl.pallas_call(
        functools.partial(kernel, chains, bonds, rows, width),
        out_shape=(
            jax.ShapeDtypeStruct(flat.shape, jnp.float32),
            jax.ShapeDtypeStruct((8, LANES), jnp.float32),
        ),
        in_specs=[pl.BlockSpec(memory_space=pltpu.HBM)] * 2,
        out_specs=(pl.BlockSpec(memory_space=pl.ANY), pl.BlockSpec(memory_space=pltpu.VMEM)),
        scratch_shapes=[
            pltpu.SemaphoreType.REGULAR,
            pltpu.SemaphoreType.REGULAR,
            dma,
            pltpu.VMEM(flat.shape, jnp.float32),
            pltpu.VMEM((2, 4 * width, LANES), jnp.float32),
            pltpu.VMEM((2,) + bond_gates.shape, jnp.float32),
            pltpu.VMEM((2 * width, width), jnp.float32),
            pltpu.VMEM((2 * width, width), jnp.float32),
            pltpu.VMEM((2, 4 * width, LANES), jnp.float32),
            pltpu.VMEM((slabs * RING, 1, LANES), jnp.float32),
            pltpu.VMEM((8, LANES), jnp.float32),
            *half,
            pltpu.VMEM(wide, jnp.float32),
            dma((2, 2, bonds // RING)), dma((2, bonds)),
            dma, dma((2,)),
            dma((GROUPS,)), dma((GROUPS,)),
            dma((2, RING)), dma((4,)),
            dma((slabs * RING,)), dma((slabs * RING,)),
            dma, dma,
        ],
        compiler_params=pltpu.CompilerParams(
            has_side_effects=True, collective_id=0, vmem_limit_bytes=56_000_000
        ),
    )(flat, pltpu.with_memory_space_constraint(bond_gates, pltpu.HBM))
    out, profile = pl.pallas_call(
        finish,
        out_shape=(
            jax.ShapeDtypeStruct(flat.shape, jnp.float32),
            jax.ShapeDtypeStruct((sites,), jnp.float32),
        ),
        in_specs=[pl.BlockSpec(memory_space=pltpu.VMEM)] * 2,
        out_specs=(pl.BlockSpec(memory_space=pl.ANY), pl.BlockSpec(memory_space=pl.ANY)),
        scratch_shapes=[pltpu.VMEM((sites,), jnp.float32), pltpu.SemaphoreType.DMA((PIECES,)), pltpu.SemaphoreType.DMA],
        compiler_params=pltpu.CompilerParams(vmem_limit_bytes=2_000_000),
    )(out, profile)
    cut = (sites, rows, width // LANES, spins, LANES)
    state = out.reshape(cut).transpose(0, 1, 3, 2, 4).reshape(site_tensors.shape)
    return (state, profile)


def solution(mesh):
    chains, bonds = (mesh.shape["chain"], mesh.shape["bond"])
    return jax.shard_map(
        functools.partial(per_device, chains, bonds),
        mesh=mesh,
        in_specs=(P("chain", "bond", None, None), P("chain", None, None)),
        out_specs=(P("chain", "bond", None, None), P("chain")),
        check_vma=False,
    )
```

```python
import functools
import math

import jax
import jax.numpy as jnp
from jax import lax
from jax.experimental import pallas as pl
from jax.experimental.pallas import tpu as pltpu
from jax.sharding import PartitionSpec as P

NS_ITERS = 3
RING = 4
GROUPS = 4
PIECES = 1
LANES = 128
EPSILON = 1e-06


def split(value):
    high = value.astype(jnp.bfloat16)
    low = (value - high.astype(jnp.float32)).astype(jnp.bfloat16)
    return (high, low)


def dot(a, b):
    return jnp.dot(a, b, preferred_element_type=jnp.float32)


def dot_t(a, b):
    return lax.dot_general(a, b, (((1,), (1,)), ((), ())), preferred_element_type=jnp.float32)


def times(a, b):
    (ah, al), (bh, bl) = (a, b)
    return dot(ah, bh) + dot(al, bh) + dot(ah, bl)


def times_transposed(a, b):
    (ah, al), (bh, bl) = (a, b)
    return dot_t(ah, bh) + dot_t(al, bh) + dot_t(ah, bl)


def mixed(theta, gate, width):
    r = theta.shape[0] // 2
    theta = [[theta[u * r:(u + 1) * r, v * width:(v + 1) * width] for v in range(2)] for u in range(2)]
    scaled = gate * (1.0 / math.sqrt(width))
    rows = []
    for s in range(2):
        row = []
        for t in range(2):
            total = None
            for u in range(2):
                for v in range(2):
                    factor = scaled[2 * s + t:2 * s + t + 1, 2 * u + v:2 * u + v + 1]
                    term = factor * theta[u][v]
                    total = term if total is None else total + term
            row.append(total)
        rows.append(jnp.concatenate(row, axis=1))
    return jnp.concatenate(rows, axis=0)


def newton_schulz(gram, fill=()):
    assert NS_ITERS == 3
    fill = list(fill)

    def filled(value):
        if fill:
            fill.pop(0)()
        return value

    eye = jnp.where(
        lax.broadcasted_iota(jnp.int32, gram.shape, 0) == lax.broadcasted_iota(jnp.int32, gram.shape, 1),
        jnp.float32(1.5),
        jnp.float32(0.0),
    )
    factor = None
    for repeat in range(NS_ITERS):
        step = eye - 0.5 * gram
        factor = step if factor is None else times(split(factor), split(step))
        if repeat < NS_ITERS - 1:
            gram_split = split(gram)
            once = 1.5 * gram - 0.5 * filled(times(gram_split, gram_split))
            gram = 1.5 * once - 0.5 * filled(times(split(once), gram_split))
    while fill:
        fill.pop(0)()
    return split(factor)


def sum_of_squares(value):
    return jnp.sum(value * value, keepdims=True)


def norm_of(carried):
    mean = sum_of_squares(carried) * (1.0 / carried.size)
    return jnp.sqrt(mean + EPSILON)


def order(place):
    return place + (place // 2) * (1 - 2 * (place % 2))


def grouped(mine, d):
    if d == 0:
        return mine
    if d == 1:
        return mine + 1 - 2 * (mine % 2)
    if d == 2:
        return lax.rem(mine + 2, 4)
    return 3 - mine


def kernel(
    chains, bonds, rows, width,
    x_ref, gates_ref, out_ref, profile_ref,
    slab_sem, ring_sem, fetch_sem, xin, inbuf, gates, rsend, rrecv, obuf, wall, below,
    bh, bl, th, tl, mh, ml, ph, pl_, lh, ll, nh, nl, uh, ul, kept,
    g_send, g_recv, gate_send, gate_recv,
    m_send, m_recv, o_send, o_recv, w_send, w_recv, p_send, p_recv,
    held, turn, d_send, d_recv, e_send, t_send, t_recv, u_send,
):
    chain, bond = (lax.axis_index("chain"), lax.axis_index("bond"))
    slabs = chains // 2
    slab, core = (chain // 2, chain % 2)
    tall = rows * 4
    part = bonds // GROUPS
    tier = width // GROUPS
    half = width // 2
    replica = bond // RING
    ring = order(bond % RING)
    block = ring // 2

    def on(which):
        return pl.when(core == which)

    def at(slab_at, core_at, bond_at):
        return {"chain": 2 * slab_at + core_at, "bond": bond_at}

    def remote(src, dst, send, recv_sem, to):
        return pltpu.make_async_remote_copy(
            src_ref=src, dst_ref=dst, send_sem=send, recv_sem=recv_sem,
            device_id=to, device_id_type=pl.DeviceIdType.MESH,
        )

    def landed(ref, sem):
        pltpu.make_async_copy(ref, ref, sem).wait()

    def greet(semaphore, to):
        pl.semaphore_signal(semaphore, inc=1, device_id=to, device_id_type=pl.DeviceIdType.MESH)

    fetch = pltpu.make_async_copy(x_ref, xin, fetch_sem)
    fetch.start()
    gate_here = pltpu.make_async_copy(gates_ref, gates.at[1], gate_recv.at[1])
    gate_copy = remote(gates_ref, gates.at[0], gate_send, gate_recv.at[0], at(slab, 1, bond))
    barrier = pltpu.get_barrier_semaphore()

    @on(1)
    def _():
        gate_here.start()
        for db in range(1, bonds):
            greet(barrier, at(slab, 1, lax.rem(bond + db, bonds)))

    @on(0)
    def _():
        greet(barrier, at(slab, 1, bond))
        for db in range(1, RING):
            greet(barrier, at(slab, 0, replica * RING + lax.rem(bond + db, RING)))

    for dz in range(1, slabs):
        for db in range(RING):
            greet(barrier, at(lax.rem(slab + dz, slabs), 0, replica * RING + lax.rem(bond + db, RING)))

    @on(1)
    def _():
        pl.semaphore_wait(barrier, bonds)
        greet(slab_sem, at(slab, 0, bond))

    @on(0)
    def _():
        pl.semaphore_wait(slab_sem, 1)

    fetch.wait()
    gathers = []
    for i in (1, 0):
        for j in range(2):
            for r in range(bonds // RING):
                bond_to = r * RING + order(2 * core + j)
                src = xin.at[pl.ds((2 * j + i) * tall, tall)]
                dst = inbuf.at[i, pl.ds(bond * tall, tall)]
                sem = g_recv.at[i, bond]
                copy = remote(src, dst, g_send.at[i, j, r], sem, at(slab, 1, bond_to))
                here = pltpu.make_async_copy(src, dst, sem)
                mine = jnp.logical_and(core == 1, bond_to == bond)
                gathers.append((copy, here, mine))
                pl.when(jnp.logical_not(mine))(copy.start)
    for copy, here, mine in gathers:
        pl.when(mine)(here.start)

    def gathers_sent():
        for copy, here, mine in gathers:
            pl.when(jnp.logical_not(mine))(copy.wait_send)

    def outputs_landed():
        for slot in range(4):
            landed(out_ref.at[pl.ds(slot * tall, tall)], o_recv.at[slot])

    @on(0)
    def _():
        gate_copy.start()
        pl.semaphore_wait(barrier, RING - 1 + (slabs - 1) * 2 * RING)
        greet(ring_sem, at(slab, 1, bond))
        gathers_sent()
        gate_copy.wait_send()
        outputs_landed()
        landed(profile_ref, p_recv)

    def gathered(i, d):
        for e in range(part):
            origin = grouped(bond // part, d) * part + lax.rem(bond + e, part)
            landed(inbuf.at[i, pl.ds(origin * tall, tall)], g_recv.at[i, origin])

    def spin(i, s, row, count):
        return jnp.concatenate(
            [inbuf[i, pl.ds(4 * row + 2 * t + s, count, stride=4), :] for t in range(2)], axis=1
        )

    @on(1)
    def _():
        before = lax.rem(ring + RING - 1, RING)
        slab_to = lax.rem(slab + slabs - jnp.where(ring == 0, 1, 0), slabs)
        previous = at(slab_to, 1, replica * RING + order(before))
        next_bond = replica * RING + order(lax.rem(ring + 1, RING))

        for d in range(GROUPS):
            gathered(1, d)
        landed(gates.at[0], gate_recv.at[0])
        landed(gates.at[1], gate_recv.at[1])
        right = jnp.concatenate([spin(1, s, 0, width) for s in range(2)], axis=1)
        bh[...], bl[...] = split(right)
        th[...], tl[...] = split(right.T)
        pl.semaphore_wait(ring_sem, 1)

        gate = gates[block, 2 * (ring % 2)]
        passed = []
        squares = None
        for d in range(GROUPS):
            g = grouped(bond // part, d)
            gathered(0, d)
            left = jnp.concatenate([spin(0, s, g * tier, tier) for s in range(2)], axis=0)
            theta = times(split(left), (bh[...], bl[...]))
            matrix = split(mixed(theta, gate, width))
            here = pl.ds(d * 2 * tier, 2 * tier)
            mh[here, :], ml[here, :] = matrix
            projected = times(matrix, (th[...], tl[...]))
            piece = pl.ds(g * 2 * tier, 2 * tier)
            rsend[piece, :] = projected
            copy = remote(rsend.at[piece], rrecv.at[piece], m_send.at[d], m_recv.at[d], previous)
            copy.start()
            passed.append(copy)
            square = sum_of_squares(projected)
            squares = square if squares is None else squares + square
            ph[:, here], pl_[:, here] = split(projected.T)

        turned = (ph[...], pl_[...])
        inverse = 1.0 / (squares + EPSILON)
        gram = times_transposed(turned, turned) * inverse
        root = jnp.sqrt(inverse)

        def carry_even(q):
            here = slice(q // 2 * width, (q // 2 + 1) * width)
            there = slice(q % 2 * half, (q % 2 + 1) * half)
            kept[there, here] = times((ph[there, :], pl_[there, :]), (mh[:, here], ml[:, here])) * root

        factor = newton_schulz(gram, [functools.partial(carry_even, q) for q in range(4)])
        carried = times(factor, split(kept[...]))
        scale_norm = norm_of(carried)
        weight_even = jnp.log(scale_norm)
        carried = split(carried * (1.0 / scale_norm))
        for s in range(2):
            lh[s * width:(s + 1) * width, :] = carried[0][:, s * width:(s + 1) * width]
            ll[s * width:(s + 1) * width, :] = carried[1][:, s * width:(s + 1) * width]

        gram = None
        squares = None
        for d in range(1, GROUPS, 2):
            parts = []
            for e in (d - 1, d):
                g = grouped(next_bond // part, e)
                piece = pl.ds(g * 2 * tier, 2 * tier)
                landed(rrecv.at[piece], m_recv.at[e])
                parts.append(rrecv[piece, :])
            received = jnp.concatenate(parts, axis=0)
            square = sum_of_squares(received)
            squares = square if squares is None else squares + square
            turned = split(received.T)
            piece = split(received)
            for k, (e, s) in enumerate([(e, s) for e in (d - 1, d) for s in range(2)]):
                g = grouped(next_bond // part, e)
                nh[pl.ds(s * width + g * tier, tier), :] = piece[0][k * tier:(k + 1) * tier]
                nl[pl.ds(s * width + g * tier, tier), :] = piece[1][k * tier:(k + 1) * tier]
            product = times(turned, piece)
            gram = product if gram is None else gram + product
        inverse = 1.0 / (squares + EPSILON)
        gate = gates[block, 2 * (ring % 2) + 1]

        def ahead(q):
            left = tuple(
                jnp.concatenate([ref[s * width + q * tier:s * width + (q + 1) * tier, :] for s in range(2)], axis=0)
                for ref in (lh, ll)
            )
            theta = [times(left, (nh[t * width:(t + 1) * width, :], nl[t * width:(t + 1) * width, :])) for t in range(2)]
            value = split(mixed(jnp.concatenate(theta, axis=1), gate, width))
            for s in range(2):
                here = slice(q // 2 * width + s * half + q % 2 * tier, q // 2 * width + s * half + (q % 2 + 1) * tier)
                uh[here, :], ul[here, :] = (part[s * tier:(s + 1) * tier] for part in value)

        factor = newton_schulz(gram * inverse, [functools.partial(ahead, q) for q in range(4)])
        scale = math.sqrt(2 * width) * jnp.sqrt(inverse)
        for t in range(2):
            value = times((nh[t * width:(t + 1) * width, :], nl[t * width:(t + 1) * width, :]), factor) * scale
            bh[:, t * width:(t + 1) * width], bl[:, t * width:(t + 1) * width] = split(value)

        right = (bh[...], bl[...])
        squares = None
        for q in range(2):
            here = slice(q * width, (q + 1) * width)
            matrix = []
            for t in range(2):
                there = slice(t * width, (t + 1) * width)
                matrix.append(times((uh[here, there], ul[here, there]), factor) * scale)
            matrix = split(jnp.concatenate(matrix, axis=1))
            mh[here, :], ml[here, :] = matrix
            projected = times_transposed(matrix, right)
            square = sum_of_squares(projected)
            squares = square if squares is None else squares + square
            ph[:, here], pl_[:, here] = split(projected.T)
            piece = split(projected)
            for s in range(2):
                to = slice(s * width + q * half, s * width + (q + 1) * half)
                nh[to, :] = piece[0][s * half:(s + 1) * half]
                nl[to, :] = piece[1][s * half:(s + 1) * half]
        turned = (ph[...], pl_[...])
        inverse = 1.0 / (squares + EPSILON)
        gram = times_transposed(turned, turned) * inverse
        root = jnp.sqrt(inverse)

        def carry(q):
            here = slice(q // 2 * width, (q // 2 + 1) * width)
            there = slice(q % 2 * half, (q % 2 + 1) * half)
            kept[there, here] = times((ph[there, :], pl_[there, :]), (mh[:, here], ml[:, here])) * root

        factor = newton_schulz(gram, [functools.partial(carry, q) for q in range(4)])

        crossing = ring == RING - 1
        across, opposite = (grouped(bond % RING, d) for d in (1, 3))
        swapped = ring % 2
        targets = [
            grouped(bond % RING, 2),
            opposite + swapped * (1 - crossing.astype(jnp.int32)) * (across - opposite),
            across + swapped * (1 - crossing.astype(jnp.int32)) * (opposite - across),
            bond % RING,
        ]
        beside = replica * RING + grouped(bond % RING, 1)
        short = tall // 2
        detours = [
            remote(
                obuf.at[1, pl.ds(beside * tall + c * short, short)], held.at[pl.ds(c * short, short)],
                d_send.at[c], d_recv.at[c], at(slab, 1, beside),
            )
            for c in range(2)
        ]
        relaying = ring == RING - 2
        relays = [
            remote(
                held.at[pl.ds(c * short, short)], out_ref.at[pl.ds(c * short, short)],
                e_send.at[c], o_recv.at[0], at(lax.rem(slab + 1, slabs), 0, bond),
            )
            for c in range(2)
        ]

        def output(h):
            site = lax.rem(slab * 2 * RING + 2 * ring + 1 + h, 4 * chains)
            chain_to, slot = (site // 4, site % 4)
            made = []
            for k in range(RING):
                bond_to = replica * RING + targets[k]
                src = obuf.at[h, pl.ds(bond_to * tall, tall)]
                dst = out_ref.at[pl.ds(slot * tall, tall)]
                copy = remote(src, dst, o_send.at[h, k], o_recv.at[slot], {"chain": chain_to, "bond": bond_to})
                here = pltpu.make_async_copy(src, dst, o_recv.at[slot])
                made.append((copy, here, chain_to == chain))
            return made

        outs = [output(h) for h in range(2)]

        def put(h):
            if h == 1:
                for copy in detours:
                    pl.when(crossing)(copy.start)
            for k, (copy, here, mine) in enumerate(outs[h]):
                if k == RING - 1:
                    pl.when(mine)(here.start)
                    pl.when(jnp.logical_not(mine))(copy.start)
                elif k == RING - 2 and h == 1:
                    pl.when(jnp.logical_not(crossing))(copy.start)
                else:
                    copy.start()

        def left_out():
            value = times((nh[...], nl[...]), factor) * (math.sqrt(2 * width) * root)
            for s in range(2):
                for t in range(2):
                    obuf[0, pl.ds(2 * t + s, width, stride=4), :] = (
                        value[s * width:(s + 1) * width, t * LANES:(t + 1) * LANES]
                    )
            put(0)

        pl.when(jnp.logical_not(crossing))(left_out)
        carried = times(factor, split(kept[...]))
        scale_norm = norm_of(carried)
        weight_odd = jnp.log(scale_norm)
        new_right = carried * (1.0 / scale_norm)

        lane = lax.broadcasted_iota(jnp.int32, (1, LANES), 1)
        odd = lane // (LANES // 2)
        own = wall.at[slab * RING + ring]
        own[...] = jnp.where(odd == 0, weight_even, weight_odd)
        weights = []
        for dz in range(slabs):
            for dk in range(RING):
                if dz == 0 and dk == 0:
                    continue
                to = at(lax.rem(slab + dz, slabs), 1, replica * RING + order(lax.rem(ring + dk, RING)))
                k = dz * RING + dk
                copy = remote(own, own, w_send.at[k], w_recv.at[k], to)
                pl.when(slab + dz < slabs)(copy.start)
                weights.append((copy, dz, dk))
        for s in range(2):
            for t in range(2):
                obuf[1, pl.ds(2 * t + s, width, stride=4), :] = (
                    new_right[:, s * width + t * LANES:s * width + (t + 1) * LANES]
                )
        put(1)
        pl.when(crossing)(left_out)

        @pl.when(relaying)
        def _():
            for c in range(2):
                landed(held.at[pl.ds(c * short, short)], d_recv.at[c])
                relays[c].start()

        for copy, dz, dk in weights:
            source = lax.rem(slab + slabs - dz, slabs) * RING + lax.rem(ring + RING - dk, RING)

            @pl.when(slab >= dz)
            def _():
                landed(wall.at[source], w_recv.at[dz * RING + dk])
        totals = [jnp.zeros((1, LANES), jnp.float32) for _ in range(2)]
        for e in range(slabs * RING):
            for c in range(2):
                counted = 2 * e + odd <= 4 * (2 * slab + c) + lane % (LANES // 2)
                totals[c] = totals[c] + jnp.where(counted, wall[e], 0.0)
        running = [
            jnp.broadcast_to((total + pltpu.roll(total, LANES // 2, 1)) * (1.0 / (4 * chains)), (8, LANES))
            for total in totals
        ]
        below[...] = running[0]
        profile_ref[...] = running[1]
        lower = remote(below, profile_ref, p_send, p_recv, at(slab, 0, bond))
        lower.start()

        outputs_landed()
        gathers_sent()
        for copy in passed + [lower]:
            copy.wait_send()
        for copy in detours:
            pl.when(crossing)(copy.wait_send)
        for copy in relays:
            pl.when(relaying)(copy.wait_send)
        for copy, dz, dk in weights:
            pl.when(slab + dz < slabs)(copy.wait_send)
        for h in range(2):
            for k, (copy, here, mine) in enumerate(outs[h]):
                if k == RING - 1:
                    pl.when(jnp.logical_not(mine))(copy.wait_send)
                elif k == RING - 2 and h == 1:
                    pl.when(jnp.logical_not(crossing))(copy.wait_send)
                else:
                    copy.wait_send()


def finish(out_ref, weights_ref, state_ref, profile_ref, held, state_sem, profile_sem):
    held[...] = weights_ref[0, :held.shape[0]]
    last = pltpu.make_async_copy(held, profile_ref, profile_sem)
    last.start()
    size = out_ref.shape[0] // PIECES
    copies = []
    for k in range(PIECES):
        here = pl.ds(k * size, size)
        copy = pltpu.make_async_copy(out_ref.at[here], state_ref.at[here], state_sem.at[k])
        copy.start()
        copies.append(copy)
    for copy in copies:
        copy.wait()
    last.wait()


def per_device(chains, bonds, site_tensors, bond_gates):
    sites, rows, spins, width = site_tensors.shape
    assert sites == 4 and spins == 2 and width == 2 * LANES and bonds % RING == 0 and chains % 2 == 0
    cut = (sites, rows, spins, width // LANES, LANES)
    flat = site_tensors.reshape(cut).transpose(0, 1, 3, 2, 4).reshape(sites * rows * 4, LANES)
    slabs = chains // 2
    dma = pltpu.SemaphoreType.DMA
    wide, tall = ((width, 2 * width), (2 * width, width))
    half = [pltpu.VMEM(shape, jnp.bfloat16) for shape in (wide, wide, tall, tall, (2 * width, 2 * width), (2 * width, 2 * width), wide, wide, tall, tall, tall, tall, (2 * width, 2 * width), (2 * width, 2 * width))]
    out, profile = pl.pallas_call(
        functools.partial(kernel, chains, bonds, rows, width),
        out_shape=(
            jax.ShapeDtypeStruct(flat.shape, jnp.float32),
            jax.ShapeDtypeStruct((8, LANES), jnp.float32),
        ),
        in_specs=[pl.BlockSpec(memory_space=pltpu.HBM)] * 2,
        out_specs=(pl.BlockSpec(memory_space=pl.ANY), pl.BlockSpec(memory_space=pltpu.VMEM)),
        scratch_shapes=[
            pltpu.SemaphoreType.REGULAR,
            pltpu.SemaphoreType.REGULAR,
            dma,
            pltpu.VMEM(flat.shape, jnp.float32),
            pltpu.VMEM((2, 4 * width, LANES), jnp.float32),
            pltpu.VMEM((2,) + bond_gates.shape, jnp.float32),
            pltpu.VMEM((2 * width, width), jnp.float32),
            pltpu.VMEM((2 * width, width), jnp.float32),
            pltpu.VMEM((2, 4 * width, LANES), jnp.float32),
            pltpu.VMEM((slabs * RING, 1, LANES), jnp.float32),
            pltpu.VMEM((8, LANES), jnp.float32),
            *half,
            pltpu.VMEM(wide, jnp.float32),
            dma((2, 2, bonds // RING)), dma((2, bonds)),
            dma, dma((2,)),
            dma((GROUPS,)), dma((GROUPS,)),
            dma((2, RING)), dma((4,)),
            dma((slabs * RING,)), dma((slabs * RING,)),
            dma, dma,
            pltpu.VMEM((rows * 4, LANES), jnp.float32),
            pltpu.VMEM((2 * width // GROUPS, width), jnp.float32),
            dma((2,)), dma((2,)), dma((2,)), dma, dma, dma,
        ],
        compiler_params=pltpu.CompilerParams(
            has_side_effects=True, collective_id=0, vmem_limit_bytes=56_000_000
        ),
    )(flat, pltpu.with_memory_space_constraint(bond_gates, pltpu.HBM))
    out, profile = pl.pallas_call(
        finish,
        out_shape=(
            jax.ShapeDtypeStruct(flat.shape, jnp.float32),
            jax.ShapeDtypeStruct((sites,), jnp.float32),
        ),
        in_specs=[pl.BlockSpec(memory_space=pltpu.VMEM)] * 2,
        out_specs=(pl.BlockSpec(memory_space=pl.ANY), pl.BlockSpec(memory_space=pl.ANY)),
        scratch_shapes=[pltpu.VMEM((sites,), jnp.float32), pltpu.SemaphoreType.DMA((PIECES,)), pltpu.SemaphoreType.DMA],
        compiler_params=pltpu.CompilerParams(vmem_limit_bytes=2_000_000),
    )(out, profile)
    cut = (sites, rows, width // LANES, spins, LANES)
    state = out.reshape(cut).transpose(0, 1, 3, 2, 4).reshape(site_tensors.shape)
    return (state, profile)


def solution(mesh):
    chains, bonds = (mesh.shape["chain"], mesh.shape["bond"])
    return jax.shard_map(
        functools.partial(per_device, chains, bonds),
        mesh=mesh,
        in_specs=(P("chain", "bond", None, None), P("chain", None, None)),
        out_specs=(P("chain", "bond", None, None), P("chain")),
        check_vma=False,
    )
```

```python
import functools
import math

import jax
import jax.numpy as jnp
from jax import lax
from jax.experimental import pallas as pl
from jax.experimental.pallas import tpu as pltpu
from jax.sharding import PartitionSpec as P

NS_ITERS = 3
RING = 4
GROUPS = 4
PIECES = 1
LANES = 128
EPSILON = 1e-06


def split(value):
    high = value.astype(jnp.bfloat16)
    low = (value - high.astype(jnp.float32)).astype(jnp.bfloat16)
    return (high, low)


def dot(a, b):
    return jnp.dot(a, b, preferred_element_type=jnp.float32)


def dot_t(a, b):
    return lax.dot_general(a, b, (((1,), (1,)), ((), ())), preferred_element_type=jnp.float32)


def times(a, b):
    (ah, al), (bh, bl) = (a, b)
    return dot(ah, bh) + dot(al, bh) + dot(ah, bl)


def times_transposed(a, b):
    (ah, al), (bh, bl) = (a, b)
    return dot_t(ah, bh) + dot_t(al, bh) + dot_t(ah, bl)


def mixed(theta, gate, width):
    r = theta.shape[0] // 2
    theta = [[theta[u * r:(u + 1) * r, v * width:(v + 1) * width] for v in range(2)] for u in range(2)]
    scaled = gate * (1.0 / math.sqrt(width))
    rows = []
    for s in range(2):
        row = []
        for t in range(2):
            total = None
            for u in range(2):
                for v in range(2):
                    factor = scaled[2 * s + t:2 * s + t + 1, 2 * u + v:2 * u + v + 1]
                    term = factor * theta[u][v]
                    total = term if total is None else total + term
            row.append(total)
        rows.append(jnp.concatenate(row, axis=1))
    return jnp.concatenate(rows, axis=0)


def newton_schulz(gram, fill=()):
    assert NS_ITERS == 3
    fill = list(fill)

    def filled(value):
        if fill:
            fill.pop(0)()
        return value

    eye = jnp.where(
        lax.broadcasted_iota(jnp.int32, gram.shape, 0) == lax.broadcasted_iota(jnp.int32, gram.shape, 1),
        jnp.float32(1.5),
        jnp.float32(0.0),
    )
    step = eye - 0.5 * gram
    first, base = (split(step), split(gram))
    square, right = (times(first, first), times(first, base))
    filled(None)
    right = split(right)
    gram, cube = (times(right, first), times(split(square), right))
    filled(None)
    second = split(eye - 0.5 * gram)
    both = 1.5 * step - 0.5 * cube
    left, right = (times(split(both), second), times(second, split(gram)))
    filled(None)
    factor = 1.5 * both - 0.5 * filled(times(split(left), split(right)))
    while fill:
        fill.pop(0)()
    return split(factor)


def sum_of_squares(value):
    return jnp.sum(value * value, keepdims=True)


def norm_of(carried):
    mean = sum_of_squares(carried) * (1.0 / carried.size)
    return jnp.sqrt(mean + EPSILON)


def order(place):
    return place + (place // 2) * (1 - 2 * (place % 2))


def grouped(mine, d):
    if d == 0:
        return mine
    if d == 1:
        return mine + 1 - 2 * (mine % 2)
    if d == 2:
        return lax.rem(mine + 2, 4)
    return 3 - mine


def kernel(
    chains, bonds, rows, width,
    x_ref, gates_ref, out_ref, profile_ref,
    slab_sem, ring_sem, fetch_sem, xin, inbuf, gates, rsend, rrecv, obuf, wall, below,
    bh, bl, th, tl, mh, ml, ph, pl_, lh, ll, nh, nl, uh, ul, kept,
    g_send, g_recv, gate_send, gate_recv,
    m_send, m_recv, o_send, o_recv, w_send, w_recv, p_send, p_recv,
    held, turn, d_send, d_recv, e_send, t_send, t_recv, u_send,
):
    chain, bond = (lax.axis_index("chain"), lax.axis_index("bond"))
    slabs = chains // 2
    slab, core = (chain // 2, chain % 2)
    tall = rows * 4
    part = bonds // GROUPS
    tier = width // GROUPS
    half = width // 2
    replica = bond // RING
    ring = order(bond % RING)
    block = ring // 2

    def on(which):
        return pl.when(core == which)

    def at(slab_at, core_at, bond_at):
        return {"chain": 2 * slab_at + core_at, "bond": bond_at}

    def remote(src, dst, send, recv_sem, to):
        return pltpu.make_async_remote_copy(
            src_ref=src, dst_ref=dst, send_sem=send, recv_sem=recv_sem,
            device_id=to, device_id_type=pl.DeviceIdType.MESH,
        )

    def landed(ref, sem):
        pltpu.make_async_copy(ref, ref, sem).wait()

    def greet(semaphore, to):
        pl.semaphore_signal(semaphore, inc=1, device_id=to, device_id_type=pl.DeviceIdType.MESH)

    fetch = pltpu.make_async_copy(x_ref, xin, fetch_sem)
    fetch.start()
    gate_here = pltpu.make_async_copy(gates_ref, gates.at[1], gate_recv.at[1])
    gate_copy = remote(gates_ref, gates.at[0], gate_send, gate_recv.at[0], at(slab, 1, bond))
    barrier = pltpu.get_barrier_semaphore()

    @on(1)
    def _():
        gate_here.start()
        for db in range(1, bonds):
            greet(barrier, at(slab, 1, lax.rem(bond + db, bonds)))

    @on(0)
    def _():
        greet(barrier, at(slab, 1, bond))
        for db in range(1, RING):
            greet(barrier, at(slab, 0, replica * RING + lax.rem(bond + db, RING)))

    for dz in range(1, slabs):
        for db in range(RING):
            greet(barrier, at(lax.rem(slab + dz, slabs), 0, replica * RING + lax.rem(bond + db, RING)))

    @on(1)
    def _():
        pl.semaphore_wait(barrier, bonds)
        greet(slab_sem, at(slab, 0, bond))

    @on(0)
    def _():
        pl.semaphore_wait(slab_sem, 1)

    fetch.wait()
    gathers = []
    for i in (1, 0):
        for j in range(2):
            for r in range(bonds // RING):
                bond_to = r * RING + order(2 * core + j)
                src = xin.at[pl.ds((2 * j + i) * tall, tall)]
                dst = inbuf.at[i, pl.ds(bond * tall, tall)]
                sem = g_recv.at[i, bond]
                copy = remote(src, dst, g_send.at[i, j, r], sem, at(slab, 1, bond_to))
                here = pltpu.make_async_copy(src, dst, sem)
                mine = jnp.logical_and(core == 1, bond_to == bond)
                gathers.append((copy, here, mine))
                pl.when(jnp.logical_not(mine))(copy.start)
    for copy, here, mine in gathers:
        pl.when(mine)(here.start)

    def gathers_sent():
        for copy, here, mine in gathers:
            pl.when(jnp.logical_not(mine))(copy.wait_send)

    def outputs_landed():
        for slot in range(4):
            landed(out_ref.at[pl.ds(slot * tall, tall)], o_recv.at[slot])

    @on(0)
    def _():
        gate_copy.start()
        pl.semaphore_wait(barrier, RING - 1 + (slabs - 1) * 2 * RING)
        greet(ring_sem, at(slab, 1, bond))
        gathers_sent()
        gate_copy.wait_send()
        outputs_landed()
        landed(profile_ref, p_recv)

    def gathered(i, d):
        for e in range(part):
            origin = grouped(bond // part, d) * part + lax.rem(bond + e, part)
            landed(inbuf.at[i, pl.ds(origin * tall, tall)], g_recv.at[i, origin])

    def spin(i, s, row, count):
        return jnp.concatenate(
            [inbuf[i, pl.ds(4 * row + 2 * t + s, count, stride=4), :] for t in range(2)], axis=1
        )

    @on(1)
    def _():
        before = lax.rem(ring + RING - 1, RING)
        slab_to = lax.rem(slab + slabs - jnp.where(ring == 0, 1, 0), slabs)
        previous = at(slab_to, 1, replica * RING + order(before))
        next_bond = replica * RING + order(lax.rem(ring + 1, RING))

        for d in range(GROUPS):
            gathered(1, d)
        landed(gates.at[0], gate_recv.at[0])
        landed(gates.at[1], gate_recv.at[1])
        pl.semaphore_wait(ring_sem, 1)
        gathered(0, 0)
        right = jnp.concatenate([spin(1, s, 0, width) for s in range(2)], axis=1)
        bh[...], bl[...] = split(right)
        th[...], tl[...] = split(right.T)

        gate = gates[block, 2 * (ring % 2)]
        passed = []
        squares = None
        for d in range(GROUPS):
            g = grouped(bond // part, d)
            if d:
                gathered(0, d)
            left = jnp.concatenate([spin(0, s, g * tier, tier) for s in range(2)], axis=0)
            theta = times(split(left), (bh[...], bl[...]))
            matrix = split(mixed(theta, gate, width))
            here = pl.ds(d * 2 * tier, 2 * tier)
            mh[here, :], ml[here, :] = matrix
            projected = times(matrix, (th[...], tl[...]))
            piece = pl.ds(g * 2 * tier, 2 * tier)
            rsend[piece, :] = projected
            copy = remote(rsend.at[piece], rrecv.at[piece], m_send.at[d], m_recv.at[d], previous)
            copy.start()
            passed.append(copy)
            square = sum_of_squares(projected)
            squares = square if squares is None else squares + square
            ph[:, here], pl_[:, here] = split(projected.T)

        turned = (ph[...], pl_[...])
        inverse = 1.0 / (squares + EPSILON)
        gram = times_transposed(turned, turned) * inverse
        root = jnp.sqrt(inverse)

        def carry_even(q):
            here = slice(q // 2 * width, (q // 2 + 1) * width)
            there = slice(q % 2 * half, (q % 2 + 1) * half)
            kept[there, here] = times((ph[there, :], pl_[there, :]), (mh[:, here], ml[:, here])) * root

        factor = newton_schulz(gram, [functools.partial(carry_even, q) for q in range(4)])
        carried = times(factor, split(kept[...]))
        scale_norm = norm_of(carried)
        weight_even = jnp.log(scale_norm)
        carried = split(carried * (1.0 / scale_norm))
        for s in range(2):
            lh[s * width:(s + 1) * width, :] = carried[0][:, s * width:(s + 1) * width]
            ll[s * width:(s + 1) * width, :] = carried[1][:, s * width:(s + 1) * width]

        gram = None
        squares = None
        pair = []
        for d in range(GROUPS):
            g = grouped(next_bond // part, d)
            piece = pl.ds(g * 2 * tier, 2 * tier)
            landed(rrecv.at[piece], m_recv.at[d])
            received = rrecv[piece, :]
            square = sum_of_squares(received)
            squares = square if squares is None else squares + square
            piece = split(received)
            for s in range(2):
                nh[pl.ds(s * width + g * tier, tier), :] = piece[0][s * tier:(s + 1) * tier]
                nl[pl.ds(s * width + g * tier, tier), :] = piece[1][s * tier:(s + 1) * tier]
            pair.append((split(received.T), piece))
            if d % 2 == 0:
                continue
            turned, piece = (
                tuple(jnp.concatenate([p[k][c] for p in pair], axis=1 - k) for c in range(2)) for k in range(2)
            )
            pair = []
            product = times(turned, piece)
            gram = product if gram is None else gram + product
        inverse = 1.0 / (squares + EPSILON)
        gate = gates[block, 2 * (ring % 2) + 1]

        def ahead(q):
            left = tuple(
                jnp.concatenate([ref[s * width + q * tier:s * width + (q + 1) * tier, :] for s in range(2)], axis=0)
                for ref in (lh, ll)
            )
            theta = [times(left, (nh[t * width:(t + 1) * width, :], nl[t * width:(t + 1) * width, :])) for t in range(2)]
            value = split(mixed(jnp.concatenate(theta, axis=1), gate, width))
            for s in range(2):
                here = slice(q // 2 * width + s * half + q % 2 * tier, q // 2 * width + s * half + (q % 2 + 1) * tier)
                uh[here, :], ul[here, :] = (part[s * tier:(s + 1) * tier] for part in value)

        factor = newton_schulz(gram * inverse, [functools.partial(ahead, q) for q in range(4)])
        scale = math.sqrt(2 * width) * jnp.sqrt(inverse)
        for t in range(2):
            value = times((nh[t * width:(t + 1) * width, :], nl[t * width:(t + 1) * width, :]), factor) * scale
            bh[:, t * width:(t + 1) * width], bl[:, t * width:(t + 1) * width] = split(value)

        right = (bh[...], bl[...])
        squares = None
        for q in range(2):
            here = slice(q * width, (q + 1) * width)
            matrix = []
            for t in range(2):
                there = slice(t * width, (t + 1) * width)
                matrix.append(times((uh[here, there], ul[here, there]), factor) * scale)
            matrix = split(jnp.concatenate(matrix, axis=1))
            mh[here, :], ml[here, :] = matrix
            projected = times_transposed(matrix, right)
            square = sum_of_squares(projected)
            squares = square if squares is None else squares + square
            ph[:, here], pl_[:, here] = split(projected.T)
            piece = split(projected)
            for s in range(2):
                to = slice(s * width + q * half, s * width + (q + 1) * half)
                nh[to, :] = piece[0][s * half:(s + 1) * half]
                nl[to, :] = piece[1][s * half:(s + 1) * half]
        turned = (ph[...], pl_[...])
        inverse = 1.0 / (squares + EPSILON)
        gram = times_transposed(turned, turned) * inverse
        root = jnp.sqrt(inverse)

        def carry(q):
            here = slice(q // 2 * width, (q // 2 + 1) * width)
            there = slice(q % 2 * half, (q % 2 + 1) * half)
            kept[there, here] = times((ph[there, :], pl_[there, :]), (mh[:, here], ml[:, here])) * root

        factor = newton_schulz(gram, [functools.partial(carry, q) for q in range(4)])

        crossing = ring == RING - 1
        across, opposite = (grouped(bond % RING, d) for d in (1, 3))
        swapped = ring % 2
        targets = [
            grouped(bond % RING, 2),
            opposite + swapped * (1 - crossing.astype(jnp.int32)) * (across - opposite),
            across + swapped * (1 - crossing.astype(jnp.int32)) * (opposite - across),
            bond % RING,
        ]
        beside = replica * RING + grouped(bond % RING, 1)
        short = tall // 2
        detours = [
            remote(
                obuf.at[1, pl.ds(beside * tall + c * short, short)], held.at[pl.ds(c * short, short)],
                d_send.at[c], d_recv.at[c], at(slab, 1, beside),
            )
            for c in range(2)
        ]
        relaying = ring == RING - 2
        relays = [
            remote(
                held.at[pl.ds(c * short, short)], out_ref.at[pl.ds(c * short, short)],
                e_send.at[c], o_recv.at[0], at(lax.rem(slab + 1, slabs), 0, bond),
            )
            for c in range(2)
        ]

        def output(h):
            site = lax.rem(slab * 2 * RING + 2 * ring + 1 + h, 4 * chains)
            chain_to, slot = (site // 4, site % 4)
            made = []
            for k in range(RING):
                bond_to = replica * RING + targets[k]
                src = obuf.at[h, pl.ds(bond_to * tall, tall)]
                dst = out_ref.at[pl.ds(slot * tall, tall)]
                copy = remote(src, dst, o_send.at[h, k], o_recv.at[slot], {"chain": chain_to, "bond": bond_to})
                here = pltpu.make_async_copy(src, dst, o_recv.at[slot])
                made.append((copy, here, chain_to == chain))
            return made

        outs = [output(h) for h in range(2)]

        def put(h):
            if h == 1:
                for copy in detours:
                    pl.when(crossing)(copy.start)
            for k, (copy, here, mine) in enumerate(outs[h]):
                if k == RING - 1:
                    pl.when(mine)(here.start)
                    pl.when(jnp.logical_not(mine))(copy.start)
                elif k == RING - 2 and h == 1:
                    pl.when(jnp.logical_not(crossing))(copy.start)
                else:
                    copy.start()

        def left_out():
            value = times((nh[...], nl[...]), factor) * (math.sqrt(2 * width) * root)
            for s in range(2):
                for t in range(2):
                    obuf[0, pl.ds(2 * t + s, width, stride=4), :] = (
                        value[s * width:(s + 1) * width, t * LANES:(t + 1) * LANES]
                    )
            put(0)

        pl.when(jnp.logical_not(crossing))(left_out)
        carried = times(factor, split(kept[...]))
        scale_norm = norm_of(carried)
        weight_odd = jnp.log(scale_norm)
        new_right = carried * (1.0 / scale_norm)

        lane = lax.broadcasted_iota(jnp.int32, (1, LANES), 1)
        odd = lane // (LANES // 2)
        own = wall.at[slab * RING + ring]
        own[...] = jnp.where(odd == 0, weight_even, weight_odd)
        weights = []
        for dz in range(slabs):
            for dk in range(RING):
                if dz == 0 and dk == 0:
                    continue
                to = at(lax.rem(slab + dz, slabs), 1, replica * RING + order(lax.rem(ring + dk, RING)))
                k = dz * RING + dk
                copy = remote(own, own, w_send.at[k], w_recv.at[k], to)
                pl.when(slab + dz < slabs)(copy.start)
                weights.append((copy, dz, dk))
        for s in range(2):
            for t in range(2):
                obuf[1, pl.ds(2 * t + s, width, stride=4), :] = (
                    new_right[:, s * width + t * LANES:s * width + (t + 1) * LANES]
                )
        put(1)
        pl.when(crossing)(left_out)

        @pl.when(relaying)
        def _():
            for c in range(2):
                landed(held.at[pl.ds(c * short, short)], d_recv.at[c])
                relays[c].start()

        for copy, dz, dk in weights:
            source = lax.rem(slab + slabs - dz, slabs) * RING + lax.rem(ring + RING - dk, RING)

            @pl.when(slab >= dz)
            def _():
                landed(wall.at[source], w_recv.at[dz * RING + dk])
        totals = [jnp.zeros((1, LANES), jnp.float32) for _ in range(2)]
        for e in range(slabs * RING):
            for c in range(2):
                counted = 2 * e + odd <= 4 * (2 * slab + c) + lane % (LANES // 2)
                totals[c] = totals[c] + jnp.where(counted, wall[e], 0.0)
        running = [
            jnp.broadcast_to((total + pltpu.roll(total, LANES // 2, 1)) * (1.0 / (4 * chains)), (8, LANES))
            for total in totals
        ]
        below[...] = running[0]
        profile_ref[...] = running[1]
        lower = remote(below, profile_ref, p_send, p_recv, at(slab, 0, bond))
        lower.start()

        outputs_landed()
        gathers_sent()
        for copy in passed + [lower]:
            copy.wait_send()
        for copy in detours:
            pl.when(crossing)(copy.wait_send)
        for copy in relays:
            pl.when(relaying)(copy.wait_send)
        for copy, dz, dk in weights:
            pl.when(slab + dz < slabs)(copy.wait_send)
        for h in range(2):
            for k, (copy, here, mine) in enumerate(outs[h]):
                if k == RING - 1:
                    pl.when(jnp.logical_not(mine))(copy.wait_send)
                elif k == RING - 2 and h == 1:
                    pl.when(jnp.logical_not(crossing))(copy.wait_send)
                else:
                    copy.wait_send()


def finish(out_ref, weights_ref, state_ref, profile_ref, held, state_sem, profile_sem):
    held[...] = weights_ref[0, :held.shape[0]]
    last = pltpu.make_async_copy(held, profile_ref, profile_sem)
    last.start()
    size = out_ref.shape[0] // PIECES
    copies = []
    for k in range(PIECES):
        here = pl.ds(k * size, size)
        copy = pltpu.make_async_copy(out_ref.at[here], state_ref.at[here], state_sem.at[k])
        copy.start()
        copies.append(copy)
    for copy in copies:
        copy.wait()
    last.wait()


def per_device(chains, bonds, site_tensors, bond_gates):
    sites, rows, spins, width = site_tensors.shape
    assert sites == 4 and spins == 2 and width == 2 * LANES and bonds % RING == 0 and chains % 2 == 0
    cut = (sites, rows, spins, width // LANES, LANES)
    flat = site_tensors.reshape(cut).transpose(0, 1, 3, 2, 4).reshape(sites * rows * 4, LANES)
    slabs = chains // 2
    dma = pltpu.SemaphoreType.DMA
    wide, tall = ((width, 2 * width), (2 * width, width))
    half = [pltpu.VMEM(shape, jnp.bfloat16) for shape in (wide, wide, tall, tall, (2 * width, 2 * width), (2 * width, 2 * width), wide, wide, tall, tall, tall, tall, (2 * width, 2 * width), (2 * width, 2 * width))]
    out, profile = pl.pallas_call(
        functools.partial(kernel, chains, bonds, rows, width),
        out_shape=(
            jax.ShapeDtypeStruct(flat.shape, jnp.float32),
            jax.ShapeDtypeStruct((8, LANES), jnp.float32),
        ),
        in_specs=[pl.BlockSpec(memory_space=pltpu.HBM)] * 2,
        out_specs=(pl.BlockSpec(memory_space=pl.ANY), pl.BlockSpec(memory_space=pltpu.VMEM)),
        scratch_shapes=[
            pltpu.SemaphoreType.REGULAR,
            pltpu.SemaphoreType.REGULAR,
            dma,
            pltpu.VMEM(flat.shape, jnp.float32),
            pltpu.VMEM((2, 4 * width, LANES), jnp.float32),
            pltpu.VMEM((2,) + bond_gates.shape, jnp.float32),
            pltpu.VMEM((2 * width, width), jnp.float32),
            pltpu.VMEM((2 * width, width), jnp.float32),
            pltpu.VMEM((2, 4 * width, LANES), jnp.float32),
            pltpu.VMEM((slabs * RING, 1, LANES), jnp.float32),
            pltpu.VMEM((8, LANES), jnp.float32),
            *half,
            pltpu.VMEM(wide, jnp.float32),
            dma((2, 2, bonds // RING)), dma((2, bonds)),
            dma, dma((2,)),
            dma((GROUPS,)), dma((GROUPS,)),
            dma((2, RING)), dma((4,)),
            dma((slabs * RING,)), dma((slabs * RING,)),
            dma, dma,
            pltpu.VMEM((rows * 4, LANES), jnp.float32),
            pltpu.VMEM((2 * width // GROUPS, width), jnp.float32),
            dma((2,)), dma((2,)), dma((2,)), dma, dma, dma,
        ],
        compiler_params=pltpu.CompilerParams(
            has_side_effects=True, collective_id=0, vmem_limit_bytes=56_000_000
        ),
    )(flat, pltpu.with_memory_space_constraint(bond_gates, pltpu.HBM))
    out, profile = pl.pallas_call(
        finish,
        out_shape=(
            jax.ShapeDtypeStruct(flat.shape, jnp.float32),
            jax.ShapeDtypeStruct((sites,), jnp.float32),
        ),
        in_specs=[pl.BlockSpec(memory_space=pltpu.VMEM)] * 2,
        out_specs=(pl.BlockSpec(memory_space=pl.ANY), pl.BlockSpec(memory_space=pl.ANY)),
        scratch_shapes=[pltpu.VMEM((sites,), jnp.float32), pltpu.SemaphoreType.DMA((PIECES,)), pltpu.SemaphoreType.DMA],
        compiler_params=pltpu.CompilerParams(vmem_limit_bytes=2_000_000),
    )(out, profile)
    cut = (sites, rows, width // LANES, spins, LANES)
    state = out.reshape(cut).transpose(0, 1, 3, 2, 4).reshape(site_tensors.shape)
    return (state, profile)


def solution(mesh):
    chains, bonds = (mesh.shape["chain"], mesh.shape["bond"])
    return jax.shard_map(
        functools.partial(per_device, chains, bonds),
        mesh=mesh,
        in_specs=(P("chain", "bond", None, None), P("chain", None, None)),
        out_specs=(P("chain", "bond", None, None), P("chain")),
        check_vma=False,
    )
```
